32 devices in a mesh: expert: 4 (over z), shard: 8 (over y, x, core).
Axes of the slice: x: 2, y: 2, z: 4, core: 2. Of those that a mesh axis runs over, the one named last changes fastest.
Arguments:
- tokens: bfloat16 [768, 4096], P(('expert', 'shard')), may hold values from -0.19921875 to 0.19921875
- expert_ids: int32 [768, 2], P(('expert', 'shard')), may hold values from 0 to 3, all different within a row; in each aligned block of 24 rows (0 to 23, 24 to 47, ...) at most 16 rows name the same one
- weight_gate: bfloat16 [4, 4096, 8192], P('expert', None, 'shard'), may hold values from -0.09375 to 0.09375
- weight_up: bfloat16 [4, 4096, 8192], P('expert', None, 'shard'), may hold values from -0.09375 to 0.09375
- gate_pre: bfloat16 [4, 512, 8192], P('expert', None, 'shard'), may hold values from -8 to 8
- up_pre: bfloat16 [4, 512, 8192], P('expert', None, 'shard'), may hold values from -6 to 6
- hidden_grad: bfloat16 [4, 512, 8192], P('expert', None, 'shard'), may hold values from -6 to 6
Outputs:
- token_grad: bfloat16 [768, 4096], P(('expert', 'shard'))
- gate_weight_grad: float32 [4, 4096, 8192], P('expert', None, 'shard')
- up_weight_grad: float32 [4, 4096, 8192], P('expert', None, 'shard')
The draws below stay inside these ranges and needn't reach their ends.
Inputs may be any that keep to these rules, and one draw needn't show every extreme that they name: `expert_ids`: each token names 2 different experts. Among the tokens of one device no expert is named more than 16 times, and in every draw some device names some expert exactly 16 times.
All inputs are finite; a program needn't handle non-finite values.
Results may differ from the reference program's by a relative error of at most 0.02.
Values may be sent and summed in bfloat16 or wider, within the bound.
A program may use at most 192 MiB of HBM per device.

```python
import math
import jax
import jax.numpy as jnp
import numpy as np
from jax import lax

D = 4096
FF = 8192
TOP = 2
TOK_DEV = 24
CAP = 16
EXPERTS = 4
TOKENS = 768
GROUP_ROWS = 512
N_EXPERT = 4
N_SHARD = 8


def shard_levels(rng, dims, split, smallest, high):
    loudness = 1.0
    for dim, shards_of in split:
        steps = jax.random.uniform(jax.random.fold_in(jax.random.fold_in(rng, 6), dim), (shards_of,), jnp.float32, smallest / len(split), high / len(split))
        loudness = loudness * jnp.repeat(jnp.exp(steps), dims[dim] // shards_of).reshape((-1,) + (1,) * (len(dims) - 1 - dim))
    return loudness


def shared_out(own_key, own, number, rows, amount, top, bound, slope):
    sequence = jax.random.permutation(own_key, amount)
    heavy_load, ordinary = load_shares(amount, rows * top, bound, slope, True), load_shares(amount, rows * top, bound, slope, False)
    places = jnp.arange(amount)

    def named(tallies, turn):
        used = int((tallies > 0).sum())
        fixed = max(1, used // 4)
        moved = fixed + (places - fixed + turn * (used - fixed)) % max(1, amount - fixed)
        return jnp.zeros((amount,), jnp.int32).at[sequence[jnp.where(places < fixed, places, moved)]].set(jnp.asarray(tallies, jnp.int32))

    tallies = jnp.where(number % 4 == 0, named(heavy_load, number // 4), named(ordinary, number - number // 4 - 1))
    mixed = jax.random.permutation(jax.random.fold_in(own, 3), amount)
    source_of, receiver = mixed[0:amount // 2 * 2:2], mixed[1:amount // 2 * 2:2]
    slack = jnp.minimum(tallies[source_of] - 1, bound - tallies[receiver]) // 2
    slack = jnp.where((source_of == sequence[0]) | (receiver == sequence[0]) | (tallies[receiver] == 0), 0, jnp.maximum(slack, 0))
    moved = jax.random.randint(jax.random.fold_in(own, 4), (amount // 2,), 0, 1 << 20) % (slack + 1)
    tallies = tallies.at[source_of].add(-moved).at[receiver].add(moved)
    items = jnp.searchsorted(jnp.cumsum(tallies), jnp.arange(rows * top), side="right").astype(jnp.int32)
    listing = items.reshape(top, rows).T
    listing = listing[jax.random.permutation(jax.random.fold_in(own, 1), rows)]
    turn = jax.random.randint(jax.random.fold_in(own, 2), (rows, 1), 0, top)
    return jnp.take_along_axis(listing, (jnp.arange(top)[None, :] + turn) % top, axis=1)


def load_shares(number_of, total, limit, skew, full):
    portions = [(1 << 20) // math.isqrt(standing ** skew) + 1 for standing in range(1, number_of + 1)]
    largest = limit if full else min(limit, max(-(-total // number_of), total * portions[0] // sum(portions)))
    least = 1 if total - largest >= number_of - 1 else 0
    given, surplus = [largest] + [least] * (number_of - 1), total - largest - least * (number_of - 1)
    while surplus > 0:
        free = [i for i in range(1, number_of) if given[i] < largest] or [i for i in range(1, number_of) if given[i] < limit]
        whole, budget = sum([portions[i] for i in free]), surplus
        for i in free:
            addition = min(limit - given[i], max(1, budget * portions[i] // whole), surplus)
            given[i] = given[i] + addition
            surplus = surplus - addition
    return np.array(given)


def centred(key, extent, spread, bound, pieces=(), held_as=jnp.bfloat16):
    gain = shard_levels(key, extent, pieces, -0.22, 0.18) if pieces else 1.0
    drawn = jax.random.normal(key, extent, jnp.float32) * spread * gain
    return jnp.minimum(jnp.maximum(drawn, -bound), bound).astype(held_as)


def setup_inputs(seed: int = 0) -> dict:
    streams_of = jax.random.split(jax.random.key(seed), 8)
    tokens = centred(streams_of[0], (TOKENS, D), 0.03, 0.19921875, ((0, 32),))
    expert_ids_keys = jax.random.split(jax.random.fold_in(streams_of[1], 1), TOKENS // TOK_DEV)
    expert_ids_turns = jax.random.permutation(jax.random.fold_in(streams_of[1], 3), TOKENS // TOK_DEV)
    expert_ids = jax.vmap(lambda own, number: shared_out(jax.random.fold_in(streams_of[1], 2), own, number, TOK_DEV, EXPERTS, TOP, CAP, 2))(expert_ids_keys, expert_ids_turns).reshape((TOKENS, TOP))
    weight_gate = centred(streams_of[2], (EXPERTS, D, FF), D ** -0.5, 0.09375, ((0, 4), (2, 8)))
    weight_up = centred(streams_of[3], (EXPERTS, D, FF), D ** -0.5, 0.09375, ((0, 4), (2, 8)))
    gate_pre = centred(streams_of[4], (EXPERTS, GROUP_ROWS, FF), 1.5, 8.0, ((0, 4), (2, 8)))
    up_pre = centred(streams_of[5], (EXPERTS, GROUP_ROWS, FF), 1.0, 6.0, ((0, 4), (2, 8)))
    hidden_grad = centred(streams_of[6], (EXPERTS, GROUP_ROWS, FF), 1.0, 6.0, ((0, 4), (2, 8)))
    return {"tokens": tokens, "expert_ids": expert_ids, "weight_gate": weight_gate, "weight_up": weight_up, "gate_pre": gate_pre, "up_pre": up_pre, "hidden_grad": hidden_grad}


def swiglu_grads(gate_values, up_values, hidden_cotangent):
    gate_float = gate_values.astype(jnp.float32)
    up_float = up_values.astype(jnp.float32)
    cotangent = hidden_cotangent.astype(jnp.float32)
    sigmoid_gate = jax.nn.sigmoid(gate_float)
    gate_grad = (cotangent * up_float * sigmoid_gate * (1.0 + gate_float * (1.0 - sigmoid_gate))).astype(jnp.bfloat16)
    up_grad = (cotangent * gate_float * sigmoid_gate).astype(jnp.bfloat16)
    return gate_grad, up_grad


def reference(tokens, expert_ids, weight_gate, weight_up, gate_pre, up_pre, hidden_grad):
    devices_all = N_EXPERT * N_SHARD
    width = tokens.shape[1]
    labels = jnp.arange(N_EXPERT, dtype=jnp.int32)
    one_hot = (expert_ids[:, :, None] == labels[None, None, :]).astype(jnp.int32)
    per_device = one_hot.reshape(devices_all, TOK_DEV * TOP, N_EXPERT)
    earlier = jnp.cumsum(per_device, axis=1) - per_device
    slot_index = jnp.sum(per_device * earlier, axis=2).reshape(TOKENS, TOP).astype(jnp.int32)
    token_index = jnp.arange(TOKENS, dtype=jnp.int32)
    device_index = token_index // TOK_DEV
    source_group = device_index // N_SHARD
    source_shard = device_index % N_SHARD
    row_index = ((source_shard * N_EXPERT + source_group)[:, None] * CAP + slot_index).astype(jnp.int32)
    dispatched = jnp.zeros((N_EXPERT, GROUP_ROWS, width), jnp.bfloat16)
    copies = jnp.broadcast_to(tokens[:, None, :], (TOKENS, TOP, width))
    dispatched = dispatched.at[expert_ids, row_index].set(copies)
    block_width = FF // N_SHARD
    gate_wgrads = []
    up_wgrads = []
    slot_grads = []
    for expert in range(N_EXPERT):
        gate_grad, up_grad = swiglu_grads(gate_pre[expert], up_pre[expert], hidden_grad[expert])
        rows_here = dispatched[expert]
        gate_wgrads.append(jnp.dot(rows_here.T, gate_grad, preferred_element_type=jnp.float32))
        up_wgrads.append(jnp.dot(rows_here.T, up_grad, preferred_element_type=jnp.float32))
        gate_matrix = weight_gate[expert]
        up_matrix = weight_up[expert]

        def add_block(total, block_number):
            first_unit = (block_number * block_width).astype(jnp.int32)
            gate_block = lax.dynamic_slice_in_dim(gate_grad, first_unit, block_width, 1)
            up_block = lax.dynamic_slice_in_dim(up_grad, first_unit, block_width, 1)
            gate_weights = lax.dynamic_slice_in_dim(gate_matrix, first_unit, block_width, 1)
            up_weights = lax.dynamic_slice_in_dim(up_matrix, first_unit, block_width, 1)
            block_term = jnp.dot(gate_block, gate_weights.T, preferred_element_type=jnp.float32)
            block_term = block_term + jnp.dot(up_block, up_weights.T, preferred_element_type=jnp.float32)
            return total + block_term.astype(jnp.bfloat16).astype(jnp.float32), None

        start_total = jnp.zeros((GROUP_ROWS, width), jnp.float32)
        total, unused = lax.scan(add_block, start_total, jnp.arange(N_SHARD, dtype=jnp.int32))
        slot_grads.append(total.astype(jnp.bfloat16))
    slot_all = jnp.stack(slot_grads)
    picked = slot_all[expert_ids, row_index].astype(jnp.float32)
    token_grad = jnp.sum(picked, axis=1).astype(jnp.bfloat16)
    return token_grad, jnp.stack(gate_wgrads), jnp.stack(up_wgrads)
```

```python
import functools
import jax
import jax.numpy as jnp
from jax import lax
from jax.experimental import pallas as pl
from jax.experimental.pallas import tpu as pltpu
from jax.sharding import PartitionSpec as P

MESH = pl.DeviceIdType.MESH
GATHERS = 4
SUMS = 8
AHEAD = 3
STEPS = 17
ORDER = (
    ("multiply", 0, 1), ("pair_sum", 1, 1), ("near_sum", 4, 1), ("spread", 5, 2), ("own_sum", 6, 1),
    ("forward", 7, 2), ("far", 9, 2), ("gathered", 10, 2),
)


def swiglu_grads(gate_values, up_values, hidden_cotangent):
    gate_float = gate_values.astype(jnp.float32)
    up_float = up_values.astype(jnp.float32)
    cotangent = hidden_cotangent.astype(jnp.float32)
    sigmoid_gate = jax.nn.sigmoid(gate_float)
    gate_grad = (
        cotangent * up_float * sigmoid_gate * (1.0 + gate_float * (1.0 - sigmoid_gate))
    ).astype(jnp.bfloat16)
    up_grad = (cotangent * gate_float * sigmoid_gate).astype(jnp.bfloat16)
    return (gate_grad, up_grad)


def slot_table(expert_ids, groups, capacity):
    token_count = expert_ids.shape[0]
    choices_per = expert_ids.shape[1]
    labels = lax.broadcasted_iota(jnp.int32, (1, 1, groups), 2)
    one_hot = (expert_ids[:, :, None] == labels).astype(jnp.int32)
    flat_hits = one_hot.reshape(token_count * choices_per, groups)
    earlier = jnp.cumsum(flat_hits, axis=0) - flat_hits
    slot_index = jnp.sum(flat_hits * earlier, axis=1).reshape(token_count, choices_per)
    slot_labels = lax.broadcasted_iota(jnp.int32, (1, 1, 1, capacity), 3)
    slot_hits = one_hot[:, :, :, None] * (slot_index[:, :, None, None] == slot_labels).astype(
        jnp.int32
    )
    selection = jnp.sum(slot_hits, axis=1).reshape(token_count, groups * capacity)
    return selection.astype(jnp.bfloat16)


def rows_inner(left_rows, right_rows):
    return lax.dot_general(
        left_rows, right_rows, (((0,), (0,)), ((), ())), preferred_element_type=jnp.float32
    )


def times_transposed(left_rows, weights):
    return lax.dot_general(
        left_rows, weights, (((1,), (1,)), ((), ())), preferred_element_type=jnp.float32
    )


def on_device_general(tokens, expert_ids, weight_gate, weight_up, gate_pre, up_pre, hidden_grad):
    groups = lax.axis_size("expert")
    shards = lax.axis_size("shard")
    model_width = tokens.shape[1]
    capacity = gate_pre.shape[1] // (groups * shards)
    selection = slot_table(expert_ids, groups, capacity)
    outgoing = rows_inner(selection, tokens).astype(jnp.bfloat16)
    gate_grad, up_grad = swiglu_grads(gate_pre[0], up_pre[0], hidden_grad[0])
    gate_matrix = weight_gate[0]
    up_matrix = weight_up[0]
    arrived = lax.all_to_all(
        outgoing.reshape(groups, capacity, model_width),
        "expert",
        split_axis=0,
        concat_axis=0,
        tiled=True,
    )
    block_rows = lax.all_gather(
        arrived.reshape(groups * capacity, model_width), "shard", axis=0, tiled=True
    )
    gate_rows = gate_grad
    up_rows = up_grad
    gate_wgrad = rows_inner(block_rows, gate_rows)
    up_wgrad = rows_inner(block_rows, up_rows)
    gate_rows = gate_grad
    up_rows = up_grad
    summed = lax.psum_scatter(
        (times_transposed(gate_rows, gate_matrix) + times_transposed(up_rows, up_matrix)).astype(
            jnp.bfloat16
        ),
        "shard",
        scatter_dimension=0,
        tiled=True,
    )
    outbound = summed.reshape(groups, capacity, model_width)
    returned = lax.all_to_all(outbound, "expert", split_axis=0, concat_axis=0, tiled=True)
    returned = returned.reshape(groups * capacity, model_width)
    token_grad = times_transposed(selection, returned.T).astype(jnp.bfloat16)
    return (token_grad, gate_wgrad[None], up_wgrad[None])


def slot_choice(expert_ids, groups, capacity):
    token_count = expert_ids.shape[1]
    lines = lax.broadcasted_iota(jnp.int32, (groups * capacity, token_count), 0)
    expert, slot = lines // capacity, lines % capacity
    named = jnp.logical_or(expert_ids[0:1, :] == expert, expert_ids[1:2, :] == expert)
    hits = jnp.where(named, 1.0, 0.0)
    above = lax.broadcasted_iota(jnp.int32, (token_count, token_count), 0)
    below = lax.broadcasted_iota(jnp.int32, (token_count, token_count), 1)
    before = jnp.where(above < below, 1.0, 0.0)
    earlier = jnp.dot(hits, before, preferred_element_type=jnp.float32)
    chosen = jnp.logical_and(named, earlier == slot.astype(jnp.float32))
    return jnp.where(chosen, 1.0, 0.0).astype(jnp.bfloat16)


def exchange_kernel(
    groups, capacity, expert_ids, tokens, weight_gate, weight_up, gate_pre, up_pre, hidden_grad,
    returned_out, block_rows, gate_out, up_out,
    token_buf, outgoing, weights, pre, gate_rows, up_rows, block, partial, from_core, total, from_diag,
    from_near, leaving, returned, load_sem, store_sem, send_sem, gather_sem, sum_sem, return_sem,
):
    e = lax.axis_index("expert")
    q = lax.axis_index("shard")
    core, x, y = q % 2, (q // 2) % 2, q // 4
    sib = q + 1 - 2 * core
    xn = q + 2 - 4 * x
    yn = q + 4 - 8 * y
    dg = xn + 4 - 8 * y
    rows = groups * capacity
    half = rows // 2
    slots = gate_rows.shape[0]
    wide = block.shape[2]
    slim = total.shape[2]

    def columns(c, width):
        return pl.ds(pl.multiple_of(c * width, width), width)

    def span(start, size):
        return pl.ds(pl.multiple_of(start, size), size)

    def held(c, start, size):
        return block.at[c, span(start, size), :]

    def chip_rows(c, device, low, size):
        return total.at[c, span(device // 2 * rows + low, size), :]

    def other(k):
        return (e + k) % groups

    def wait(place, sem):
        pltpu.make_async_copy(place, place, sem).wait()

    def target(k):
        if k < 3:
            return (other(k + 1), q)
        if k >= 18:
            return (other(k - 17), q)
        if k in (3, 7, 12, 14, 16):
            return (e, xn)
        if k in (4, 6, 13, 15, 17):
            return (e, yn)
        return (e, sib)

    def copy(k, c):
        if k < 3:
            source = outgoing.at[other(k + 1), :, columns(c, wide)]
            to = held(c, q * rows + e * capacity, capacity)
        elif k < 6:
            source = to = held(c, q * rows, rows)
        elif k == 6:
            source = to = held(c, xn * rows, half)
        elif k == 7:
            source = to = held(c, yn * rows + half, half)
        elif k < 11:
            source = to = held(c, (xn, yn, dg)[k - 8] * rows, rows)
        elif k == 11:
            source, to = partial.at[c, 1 - core], from_core.at[c]
        elif k == 12:
            source, to = chip_rows(c, dg, 0, half), from_diag.at[c, 0]
        elif k == 13:
            source, to = chip_rows(c, dg, half, half), from_diag.at[c, 1]
        elif k == 14:
            source, to = chip_rows(c, xn, 0, half), from_near.at[c, 0, 0]
        elif k == 15:
            source, to = chip_rows(c, yn, half, half), from_near.at[c, 1, 1]
        elif k == 16:
            source, to = chip_rows(c, xn, half, half), from_near.at[c, 0, 1]
        elif k == 17:
            source, to = chip_rows(c, yn, 0, half), from_near.at[c, 1, 0]
        else:
            source = leaving.at[c, span(other(k - 17) * capacity, capacity), :]
            to = returned.at[c, span(e * capacity, capacity), :]
        if k < 11:
            recv = gather_sem.at[c, (0, 0, 0, 1, 2, 4, 3, 3, 4, 4, 4)[k]]
        elif k < 18:
            recv = sum_sem.at[c, (0, 1, 1, 2, 2, 2, 2)[k - 11]]
        else:
            recv = return_sem.at[0]
        return pltpu.make_async_remote_copy(
            src_ref=source, dst_ref=to, send_sem=send_sem.at[0], recv_sem=recv,
            device_id=target(k), device_id_type=MESH,
        )

    def weight_loads(c):
        for i, source in enumerate((weight_gate, weight_up)):
            pltpu.make_async_copy(
                source.at[0, columns(c, slim), :], weights.at[c, i], load_sem.at[c]
            ).start()

    token_load = pltpu.make_async_copy(tokens, token_buf, load_sem.at[SUMS])
    token_load.start()
    for i, source in enumerate((gate_pre, up_pre, hidden_grad)):
        pltpu.make_async_copy(source.at[0], pre.at[i], load_sem.at[SUMS + 1]).start()
    for c in range(AHEAD):
        weight_loads(c)

    barrier = pltpu.get_barrier_semaphore()
    for device in ((other(1), q), (other(2), q), (other(3), q), (e, sib), (e, xn), (e, yn)):
        pl.semaphore_signal(barrier, inc=1, device_id=device, device_id_type=MESH)
    selection = slot_choice(expert_ids[...], groups, capacity)
    token_load.wait()
    for c in range(GATHERS):
        here = slice(c * wide, (c + 1) * wide)
        picked = jnp.dot(
            selection, token_buf[:, here], preferred_element_type=jnp.float32
        ).astype(jnp.bfloat16)
        for group in range(groups):
            outgoing[group, :, here] = picked[group * capacity : (group + 1) * capacity]

    @pl.loop(0, GATHERS)
    def _(c):
        block[c, span(q * rows + e * capacity, capacity), :] = outgoing[e, :, columns(c, wide)]

    wait(pre, load_sem.at[SUMS + 1])
    step_rows = 32

    @pl.loop(0, slots // step_rows)
    def _(i):
        here = span(i * step_rows, step_rows)
        gate_grad, up_grad = swiglu_grads(pre[0, here, :], pre[1, here, :], pre[2, here, :])
        gate_rows[here, :] = gate_grad
        up_rows[here, :] = up_grad

    for i in range(2):
        pltpu.make_async_copy(
            (gate_rows, up_rows)[i], (gate_out, up_out)[i], store_sem.at[0, i]
        ).start()

    def multiply(c):
        @pl.when(c < SUMS - AHEAD)
        def _():
            weight_loads(c + AHEAD)

        wait(weights.at[c], load_sem.at[c])
        term = times_transposed(gate_rows[...], weights[c, 0]) + times_transposed(
            up_rows[...], weights[c, 1]
        )
        term = term.astype(jnp.bfloat16)
        for chip in range(slots // (2 * rows)):
            for side in range(2):
                low = (2 * chip + side) * rows
                partial[c, side, chip * rows : (chip + 1) * rows, :] = term[low : low + rows]

        @pl.when(c == 0)
        def _():
            pl.semaphore_wait(barrier, 6)

            @pl.loop(0, GATHERS)
            def _(i):
                for k in (1, 0, 2):
                    copy(k, i).start()

        copy(11, c).start()

    def spread(c):
        wait(held(c, 0, 3 * capacity), gather_sem.at[c, 0])
        for k in (3, 4, 5):
            copy(k, c).start()

    def forward(c):
        wait(held(c, 0, rows), gather_sem.at[c, 1])
        copy(6, c).start()
        copy(8, c).start()
        wait(held(c, 0, rows), gather_sem.at[c, 2])
        copy(7, c).start()
        copy(9, c).start()

    def far(c):
        wait(held(c, 0, rows), gather_sem.at[c, 3])
        copy(10, c).start()

    def gathered(c):
        wait(held(c, 0, 4 * rows), gather_sem.at[c, 4])
        pltpu.make_async_copy(
            block.at[c], block_rows.at[:, columns(c, wide)], store_sem.at[1, c]
        ).start()

    def pair_sum(c):
        wait(from_core.at[c], sum_sem.at[c, 0])
        both = partial[c, core].astype(jnp.float32) + from_core[c].astype(jnp.float32)
        total[c] = both.astype(jnp.bfloat16)
        for k in (12, 13, 14, 15):
            copy(k, c).start()

    def near_sum(c):
        wait(from_diag.at[c], sum_sem.at[c, 1])
        for side, device, low in ((0, yn, 0), (1, xn, half)):
            place = span(device // 2 * rows + low, half)
            added = total[c, place, :].astype(jnp.float32) + from_diag[c, side].astype(jnp.float32)
            total[c, place, :] = added.astype(jnp.bfloat16)
            copy(17 if side == 0 else 16, c).start()

    def own_sum(c):
        wait(from_near.at[c], sum_sem.at[c, 2])
        for low in range(2):
            place = span(q // 2 * rows + low * half, half)
            added = total[c, place, :].astype(jnp.float32)
            added = added + from_near[c, 0, low].astype(jnp.float32)
            added = added + from_near[c, 1, low].astype(jnp.float32)
            leaving[c, low * half : (low + 1) * half, :] = added.astype(jnp.bfloat16)
        mine = span(e * capacity, capacity)
        returned[c, mine, :] = leaving[c, mine, :]
        for k in (19, 18, 20):
            copy(k, c).start()

    @pl.loop(0, STEPS)
    def _(step):
        for name, first, every in ORDER:
            stage = dict(
                multiply=multiply, pair_sum=pair_sum, near_sum=near_sum, own_sum=own_sum,
                spread=spread, forward=forward, far=far, gathered=gathered,
            )[name]
            count = GATHERS if name in ("spread", "forward", "far", "gathered") else SUMS
            c = (step - first) // every
            ready = jnp.logical_and(step >= first, step < first + every * count)
            if every > 1:
                ready = jnp.logical_and(ready, (step - first) % every == 0)

            @pl.when(ready)
            def _():
                stage(c)

    wait(returned.at[:, pl.ds(0, 3 * capacity), :], return_sem.at[0])
    for c in range(SUMS):
        pltpu.make_async_copy(
            returned.at[c], returned_out.at[:, columns(c, slim)], store_sem.at[2, 0]
        ).start()
    sent = (6 * capacity + 6 * rows + 8 * half + slots // 2) * SUMS * slim // weight_gate.shape[2]
    wait(weight_gate.at[0, pl.ds(0, sent), :], send_sem.at[0])
    for c in range(GATHERS):
        wait(block.at[c], store_sem.at[1, c])
    wait(returned, store_sem.at[2, 0])
    wait(gate_rows, store_sem.at[0, 0])
    wait(up_rows, store_sem.at[0, 1])


def weight_grad_kernel(
    groups, capacity, expert_ids, returned, block_rows, gate_rows, up_rows,
    token_grad, gate_wgrad, up_wgrad, selection,
):
    @pl.when(pl.program_id(0) == 0)
    def _():
        selection[...] = slot_choice(expert_ids[...], groups, capacity)

    left = block_rows[...]
    gate_wgrad[0] = rows_inner(left, gate_rows[...])
    up_wgrad[0] = rows_inner(left, up_rows[...])
    token_grad[...] = rows_inner(selection[...], returned[...]).astype(jnp.bfloat16)


def on_device(tokens, expert_ids, weight_gate, weight_up, gate_pre, up_pre, hidden_grad):
    groups = lax.axis_size("expert")
    shards = lax.axis_size("shard")
    token_count, model_width = tokens.shape
    slots, hidden = gate_pre.shape[1:]
    capacity = slots // (groups * shards)
    rows = groups * capacity
    wide = model_width // GATHERS
    slim = model_width // SUMS
    bf16 = jnp.bfloat16
    choices = expert_ids.T
    in_vmem = pl.BlockSpec(memory_space=pltpu.VMEM)
    anywhere = pl.BlockSpec(memory_space=pl.ANY)
    returned, block_rows, gate_rows, up_rows = pl.pallas_call(
        functools.partial(exchange_kernel, groups, capacity),
        out_shape=(
            jax.ShapeDtypeStruct((rows, model_width), bf16),
            jax.ShapeDtypeStruct((slots, model_width), bf16),
            jax.ShapeDtypeStruct((slots, hidden), bf16),
            jax.ShapeDtypeStruct((slots, hidden), bf16),
        ),
        in_specs=[in_vmem] + [anywhere] * 6,
        out_specs=(anywhere, anywhere, anywhere, anywhere),
        scratch_shapes=[
            pltpu.VMEM((token_count, model_width), bf16),
            pltpu.VMEM((groups, capacity, model_width), bf16),
            pltpu.VMEM((SUMS, 2, slim, hidden), bf16),
            pltpu.VMEM((3, slots, hidden), bf16),
            pltpu.VMEM((slots, hidden), bf16),
            pltpu.VMEM((slots, hidden), bf16),
            pltpu.VMEM((GATHERS, slots, wide), bf16),
            pltpu.VMEM((SUMS, 2, slots // 2, slim), bf16),
            pltpu.VMEM((SUMS, slots // 2, slim), bf16),
            pltpu.VMEM((SUMS, slots // 2, slim), bf16),
            pltpu.VMEM((SUMS, 2, rows // 2, slim), bf16),
            pltpu.VMEM((SUMS, 2, 2, rows // 2, slim), bf16),
            pltpu.VMEM((SUMS, rows, slim), bf16),
            pltpu.VMEM((SUMS, rows, slim), bf16),
            pltpu.SemaphoreType.DMA((SUMS + 2,)),
            pltpu.SemaphoreType.DMA((3, GATHERS)),
            pltpu.SemaphoreType.DMA((1,)),
            pltpu.SemaphoreType.DMA((GATHERS, 5)),
            pltpu.SemaphoreType.DMA((SUMS, 3)),
            pltpu.SemaphoreType.DMA((1,)),
        ],
        compiler_params=pltpu.CompilerParams(
            collective_id=0, has_side_effects=True, vmem_limit_bytes=60 * 1024 * 1024
        ),
    )(choices, tokens, weight_gate, weight_up, gate_pre, up_pre, hidden_grad)
    tile = min(512, model_width)
    wgrad_shape = jax.ShapeDtypeStruct((1, model_width, hidden), jnp.float32)
    token_grad, gate_wgrad, up_wgrad = pl.pallas_call(
        functools.partial(weight_grad_kernel, groups, capacity),
        grid=(model_width // tile,),
        out_shape=(jax.ShapeDtypeStruct((token_count, model_width), bf16), wgrad_shape, wgrad_shape),
        in_specs=[
            pl.BlockSpec(choices.shape, lambda i: (0, 0)),
            pl.BlockSpec((rows, tile), lambda i: (0, i)),
            pl.BlockSpec((slots, tile), lambda i: (0, i)),
            pl.BlockSpec((slots, hidden), lambda i: (0, 0)),
            pl.BlockSpec((slots, hidden), lambda i: (0, 0)),
        ],
        out_specs=(
            pl.BlockSpec((token_count, tile), lambda i: (0, i)),
            pl.BlockSpec((1, tile, hidden), lambda i: (0, i, 0)),
            pl.BlockSpec((1, tile, hidden), lambda i: (0, i, 0)),
        ),
        scratch_shapes=[pltpu.VMEM((rows, token_count), bf16)],
        compiler_params=pltpu.CompilerParams(vmem_limit_bytes=63 * 1024 * 1024),
    )(choices, returned, block_rows, gate_rows, up_rows)
    return (token_grad, gate_wgrad, up_wgrad)


def solution(mesh):
    placed = (
        P(("expert", "shard"), None),
        P(("expert", "shard"), None),
        P("expert", None, "shard"),
        P("expert", None, "shard"),
        P("expert", None, "shard"),
        P("expert", None, "shard"),
        P("expert", None, "shard"),
    )
    small = mesh.shape["shard"] == 8 and mesh.shape["expert"] == 4
    return jax.shard_map(
        on_device if small else on_device_general,
        mesh=mesh,
        in_specs=placed,
        out_specs=(
            P(("expert", "shard"), None),
            P("expert", None, "shard"),
            P("expert", None, "shard"),
        ),
        check_vma=False,
    )
```

```python
import functools
import jax
import jax.numpy as jnp
from jax import lax
from jax.experimental import pallas as pl
from jax.experimental.pallas import tpu as pltpu
from jax.sharding import PartitionSpec as P

MESH = pl.DeviceIdType.MESH
GATHERS = 4
SUMS = 8
AHEAD = 3
STEPS = 17
ORDER = (
    ("multiply", 0, 1),
    ("pair_sum", 1, 1),
    ("near_sum", 4, 1),
    ("spread", 5, 2),
    ("own_sum", 6, 1),
    ("forward", 7, 2),
    ("far", 9, 2),
    ("gathered", 10, 2),
)


def swiglu_grads(gate_values, up_values, hidden_cotangent):
    gate_float = gate_values.astype(jnp.float32)
    up_float = up_values.astype(jnp.float32)
    cotangent = hidden_cotangent.astype(jnp.float32)
    sigmoid_gate = jax.nn.sigmoid(gate_float)
    gate_grad = (
        cotangent * up_float * sigmoid_gate * (1.0 + gate_float * (1.0 - sigmoid_gate))
    ).astype(jnp.bfloat16)
    up_grad = (cotangent * gate_float * sigmoid_gate).astype(jnp.bfloat16)
    return (gate_grad, up_grad)


def slot_table(expert_ids, groups, capacity):
    token_count = expert_ids.shape[0]
    choices_per = expert_ids.shape[1]
    labels = lax.broadcasted_iota(jnp.int32, (1, 1, groups), 2)
    one_hot = (expert_ids[:, :, None] == labels).astype(jnp.int32)
    flat_hits = one_hot.reshape(token_count * choices_per, groups)
    earlier = jnp.cumsum(flat_hits, axis=0) - flat_hits
    slot_index = jnp.sum(flat_hits * earlier, axis=1).reshape(token_count, choices_per)
    slot_labels = lax.broadcasted_iota(jnp.int32, (1, 1, 1, capacity), 3)
    slot_hits = one_hot[:, :, :, None] * (slot_index[:, :, None, None] == slot_labels).astype(
        jnp.int32
    )
    selection = jnp.sum(slot_hits, axis=1).reshape(token_count, groups * capacity)
    return selection.astype(jnp.bfloat16)


def rows_inner(left_rows, right_rows):
    return lax.dot_general(
        left_rows, right_rows, (((0,), (0,)), ((), ())), preferred_element_type=jnp.float32
    )


def times_transposed(left_rows, weights):
    return lax.dot_general(
        left_rows, weights, (((1,), (1,)), ((), ())), preferred_element_type=jnp.float32
    )


def on_device_general(tokens, expert_ids, weight_gate, weight_up, gate_pre, up_pre, hidden_grad):
    groups = lax.axis_size("expert")
    shards = lax.axis_size("shard")
    model_width = tokens.shape[1]
    capacity = gate_pre.shape[1] // (groups * shards)
    selection = slot_table(expert_ids, groups, capacity)
    outgoing = rows_inner(selection, tokens).astype(jnp.bfloat16)
    gate_grad, up_grad = swiglu_grads(gate_pre[0], up_pre[0], hidden_grad[0])
    gate_matrix = weight_gate[0]
    up_matrix = weight_up[0]
    arrived = lax.all_to_all(
        outgoing.reshape(groups, capacity, model_width),
        "expert",
        split_axis=0,
        concat_axis=0,
        tiled=True,
    )
    block_rows = lax.all_gather(
        arrived.reshape(groups * capacity, model_width), "shard", axis=0, tiled=True
    )
    gate_rows = gate_grad
    up_rows = up_grad
    gate_wgrad = rows_inner(block_rows, gate_rows)
    up_wgrad = rows_inner(block_rows, up_rows)
    gate_rows = gate_grad
    up_rows = up_grad
    summed = lax.psum_scatter(
        (times_transposed(gate_rows, gate_matrix) + times_transposed(up_rows, up_matrix)).astype(
            jnp.bfloat16
        ),
        "shard",
        scatter_dimension=0,
        tiled=True,
    )
    outbound = summed.reshape(groups, capacity, model_width)
    returned = lax.all_to_all(outbound, "expert", split_axis=0, concat_axis=0, tiled=True)
    returned = returned.reshape(groups * capacity, model_width)
    token_grad = times_transposed(selection, returned.T).astype(jnp.bfloat16)
    return (token_grad, gate_wgrad[None], up_wgrad[None])


def slot_choice(expert_ids, groups, capacity):
    token_count = expert_ids.shape[1]
    lines = lax.broadcasted_iota(jnp.int32, (groups * capacity, token_count), 0)
    expert, slot = lines // capacity, lines % capacity
    named = jnp.logical_or(expert_ids[0:1, :] == expert, expert_ids[1:2, :] == expert)
    hits = jnp.where(named, 1.0, 0.0)
    above = lax.broadcasted_iota(jnp.int32, (token_count, token_count), 0)
    below = lax.broadcasted_iota(jnp.int32, (token_count, token_count), 1)
    before = jnp.where(above < below, 1.0, 0.0)
    earlier = jnp.dot(hits, before, preferred_element_type=jnp.float32)
    chosen = jnp.logical_and(named, earlier == slot.astype(jnp.float32))
    return jnp.where(chosen, 1.0, 0.0).astype(jnp.bfloat16)


def exchange_kernel(
    groups, capacity, expert_ids, tokens, weight_gate, weight_up, gate_pre, up_pre, hidden_grad,
    returned, block, gate_rows, up_rows, selection,
    choices, token_buf, outgoing, weights, pre, partial, from_core, total, from_diag,
    from_near, leaving, load_sem, send_sem, gather_sem, sum_sem, return_sem,
):
    e = lax.axis_index("expert")
    q = lax.axis_index("shard")
    core, x, y = q % 2, (q // 2) % 2, q // 4
    sib = q + 1 - 2 * core
    xn = q + 2 - 4 * x
    yn = q + 4 - 8 * y
    dg = xn + 4 - 8 * y
    rows = groups * capacity
    half = rows // 2
    slots = gate_rows.shape[0]
    wide = block.shape[1] // GATHERS
    slim = total.shape[2]

    def columns(c, width):
        return pl.ds(pl.multiple_of(c * width, width), width)

    def span(start, size):
        return pl.ds(pl.multiple_of(start, size), size)

    def held(c, start, size):
        return block.at[span(start, size), columns(c, wide)]

    def chip_rows(c, device, low, size):
        return total.at[c, span(device // 2 * rows + low, size), :]

    def other(k):
        return (e + k) % groups

    def wait(place, sem):
        pltpu.make_async_copy(place, place, sem).wait()

    def target(k):
        if k < 3:
            return (other(k + 1), q)
        if k >= 18:
            return (other(k - 17), q)
        if k in (3, 7, 12, 14, 16):
            return (e, xn)
        if k in (4, 6, 13, 15, 17):
            return (e, yn)
        return (e, sib)

    def copy(k, c):
        if k < 3:
            source = outgoing.at[other(k + 1), :, columns(c, wide)]
            to = held(c, q * rows + e * capacity, capacity)
        elif k < 6:
            source = to = held(c, q * rows, rows)
        elif k == 6:
            source = to = held(c, xn * rows, half)
        elif k == 7:
            source = to = held(c, yn * rows + half, half)
        elif k < 11:
            source = to = held(c, (xn, yn, dg)[k - 8] * rows, rows)
        elif k == 11:
            source, to = partial.at[c, 1 - core], from_core.at[c]
        elif k == 12:
            source, to = chip_rows(c, dg, 0, half), from_diag.at[c, 0]
        elif k == 13:
            source, to = chip_rows(c, dg, half, half), from_diag.at[c, 1]
        elif k == 14:
            source, to = chip_rows(c, xn, 0, half), from_near.at[c, 0, 0]
        elif k == 15:
            source, to = chip_rows(c, yn, half, half), from_near.at[c, 1, 1]
        elif k == 16:
            source, to = chip_rows(c, xn, half, half), from_near.at[c, 0, 1]
        elif k == 17:
            source, to = chip_rows(c, yn, 0, half), from_near.at[c, 1, 0]
        else:
            source = leaving.at[c, span(other(k - 17) * capacity, capacity), :]
            to = returned.at[span(e * capacity, capacity), columns(c, slim)]
        if k < 11:
            recv = gather_sem.at[c, (0, 0, 0, 1, 2, 4, 3, 3, 4, 4, 4)[k]]
        elif k < 18:
            recv = sum_sem.at[c, (0, 1, 1, 2, 2, 2, 2)[k - 11]]
        else:
            recv = return_sem.at[0]
        return pltpu.make_async_remote_copy(
            src_ref=source, dst_ref=to, send_sem=send_sem.at[0], recv_sem=recv,
            device_id=target(k), device_id_type=MESH,
        )

    def weight_loads(c):
        for i, source in enumerate((weight_gate, weight_up)):
            pltpu.make_async_copy(
                source.at[0, columns(c, slim), :], weights.at[c, i], load_sem.at[c]
            ).start()

    token_load = pltpu.make_async_copy(tokens, token_buf, load_sem.at[SUMS])
    token_load.start()
    choice_load = pltpu.make_async_copy(expert_ids, choices, load_sem.at[SUMS + 2])
    choice_load.start()
    for i, source in enumerate((gate_pre, up_pre, hidden_grad)):
        pltpu.make_async_copy(source.at[0], pre.at[i], load_sem.at[SUMS + 1]).start()
    for c in range(AHEAD):
        weight_loads(c)

    barrier = pltpu.get_barrier_semaphore()
    for device in ((other(1), q), (other(2), q), (other(3), q), (e, sib), (e, xn), (e, yn)):
        pl.semaphore_signal(barrier, inc=1, device_id=device, device_id_type=MESH)
    choice_load.wait()
    selection[...] = slot_choice(choices[...], groups, capacity)
    token_load.wait()
    for c in range(GATHERS):
        here = slice(c * wide, (c + 1) * wide)
        picked = jnp.dot(
            selection[...], token_buf[:, here], preferred_element_type=jnp.float32
        ).astype(jnp.bfloat16)
        for group in range(groups):
            outgoing[group, :, here] = picked[group * capacity : (group + 1) * capacity]

    @pl.loop(0, GATHERS)
    def _(c):
        here = columns(c, wide)
        block[span(q * rows + e * capacity, capacity), here] = outgoing[e, :, here]

    wait(pre, load_sem.at[SUMS + 1])
    step_rows = 32

    @pl.loop(0, slots // step_rows)
    def _(i):
        here = span(i * step_rows, step_rows)
        gate_grad, up_grad = swiglu_grads(pre[0, here, :], pre[1, here, :], pre[2, here, :])
        gate_rows[here, :] = gate_grad
        up_rows[here, :] = up_grad

    def multiply(c):
        @pl.when(c < SUMS - AHEAD)
        def _():
            weight_loads(c + AHEAD)

        wait(weights.at[c], load_sem.at[c])
        term = times_transposed(gate_rows[...], weights[c, 0]) + times_transposed(
            up_rows[...], weights[c, 1]
        )
        term = term.astype(jnp.bfloat16)
        for chip in range(slots // (2 * rows)):
            for side in range(2):
                low = (2 * chip + side) * rows
                partial[c, side, chip * rows : (chip + 1) * rows, :] = term[low : low + rows]

        @pl.when(c == 0)
        def _():
            pl.semaphore_wait(barrier, 6)

            @pl.loop(0, GATHERS)
            def _(i):
                for k in (1, 0, 2):
                    copy(k, i).start()

        copy(11, c).start()

    def spread(c):
        wait(held(c, 0, 3 * capacity), gather_sem.at[c, 0])
        for k in (3, 4, 5):
            copy(k, c).start()

    def forward(c):
        wait(held(c, 0, rows), gather_sem.at[c, 1])
        copy(6, c).start()
        copy(8, c).start()
        wait(held(c, 0, rows), gather_sem.at[c, 2])
        copy(7, c).start()
        copy(9, c).start()

    def far(c):
        wait(held(c, 0, rows), gather_sem.at[c, 3])
        copy(10, c).start()

    def gathered(c):
        wait(held(c, 0, 4 * rows), gather_sem.at[c, 4])

    def pair_sum(c):
        wait(from_core.at[c], sum_sem.at[c, 0])
        both = partial[c, core].astype(jnp.float32) + from_core[c].astype(jnp.float32)
        total[c] = both.astype(jnp.bfloat16)
        for k in (12, 13, 14, 15):
            copy(k, c).start()

    def near_sum(c):
        wait(from_diag.at[c], sum_sem.at[c, 1])
        for side, device, low in ((0, yn, 0), (1, xn, half)):
            place = span(device // 2 * rows + low, half)
            added = total[c, place, :].astype(jnp.float32) + from_diag[c, side].astype(jnp.float32)
            total[c, place, :] = added.astype(jnp.bfloat16)
            copy(17 if side == 0 else 16, c).start()

    def own_sum(c):
        wait(from_near.at[c], sum_sem.at[c, 2])
        for low in range(2):
            place = span(q // 2 * rows + low * half, half)
            added = total[c, place, :].astype(jnp.float32)
            added = added + from_near[c, 0, low].astype(jnp.float32)
            added = added + from_near[c, 1, low].astype(jnp.float32)
            leaving[c, low * half : (low + 1) * half, :] = added.astype(jnp.bfloat16)
        mine = span(e * capacity, capacity)
        returned[mine, columns(c, slim)] = leaving[c, mine, :]
        for k in (19, 18, 20):
            copy(k, c).start()

    @pl.loop(0, STEPS)
    def _(step):
        for name, first, every in ORDER:
            stage = dict(
                multiply=multiply, pair_sum=pair_sum, near_sum=near_sum, own_sum=own_sum,
                spread=spread, forward=forward, far=far, gathered=gathered,
            )[name]
            count = GATHERS if name in ("spread", "forward", "far", "gathered") else SUMS
            c = (step - first) // every
            ready = jnp.logical_and(step >= first, step < first + every * count)
            if every > 1:
                ready = jnp.logical_and(ready, (step - first) % every == 0)

            @pl.when(ready)
            def _():
                stage(c)

    wait(returned.at[pl.ds(0, 3 * capacity), :], return_sem.at[0])
    sent = (6 * capacity + 6 * rows + 8 * half + slots // 2) * SUMS * slim // weight_gate.shape[2]
    wait(weight_gate.at[0, pl.ds(0, sent), :], send_sem.at[0])


def weight_grad_kernel(
    returned, block_rows, gate_rows, up_rows, selection, token_grad, gate_wgrad, up_wgrad,
):
    tile = gate_wgrad.shape[1]
    here = pl.ds(pl.multiple_of(pl.program_id(0) * tile, tile), tile)
    left = block_rows[:, here]
    gate_wgrad[0] = rows_inner(left, gate_rows[...])
    up_wgrad[0] = rows_inner(left, up_rows[...])
    token_grad[...] = rows_inner(selection[...], returned[:, here]).astype(jnp.bfloat16)


def on_device(tokens, expert_ids, weight_gate, weight_up, gate_pre, up_pre, hidden_grad):
    groups = lax.axis_size("expert")
    shards = lax.axis_size("shard")
    token_count, model_width = tokens.shape
    slots, hidden = gate_pre.shape[1:]
    capacity = slots // (groups * shards)
    rows = groups * capacity
    slim = model_width // SUMS
    bf16 = jnp.bfloat16
    kept = [
        pltpu.with_memory_space_constraint(array, pltpu.HBM)
        for array in (expert_ids.T, tokens, weight_gate, weight_up, gate_pre, up_pre, hidden_grad)
    ]
    in_vmem = pl.BlockSpec(memory_space=pltpu.VMEM)
    in_hbm = pl.BlockSpec(memory_space=pltpu.HBM)
    returned, block_rows, gate_rows, up_rows, selection = pl.pallas_call(
        functools.partial(exchange_kernel, groups, capacity),
        out_shape=(
            jax.ShapeDtypeStruct((rows, model_width), bf16),
            jax.ShapeDtypeStruct((slots, model_width), bf16),
            jax.ShapeDtypeStruct((slots, hidden), bf16),
            jax.ShapeDtypeStruct((slots, hidden), bf16),
            jax.ShapeDtypeStruct((rows, token_count), bf16),
        ),
        in_specs=[in_hbm] * 7,
        out_specs=(in_vmem,) * 5,
        scratch_shapes=[
            pltpu.VMEM(expert_ids.shape[::-1], expert_ids.dtype),
            pltpu.VMEM((token_count, model_width), bf16),
            pltpu.VMEM((groups, capacity, model_width), bf16),
            pltpu.VMEM((SUMS, 2, slim, hidden), bf16),
            pltpu.VMEM((3, slots, hidden), bf16),
            pltpu.VMEM((SUMS, 2, slots // 2, slim), bf16),
            pltpu.VMEM((SUMS, slots // 2, slim), bf16),
            pltpu.VMEM((SUMS, slots // 2, slim), bf16),
            pltpu.VMEM((SUMS, 2, rows // 2, slim), bf16),
            pltpu.VMEM((SUMS, 2, 2, rows // 2, slim), bf16),
            pltpu.VMEM((SUMS, rows, slim), bf16),
            pltpu.SemaphoreType.DMA((SUMS + 3,)),
            pltpu.SemaphoreType.DMA((1,)),
            pltpu.SemaphoreType.DMA((GATHERS, 5)),
            pltpu.SemaphoreType.DMA((SUMS, 3)),
            pltpu.SemaphoreType.DMA((1,)),
        ],
        compiler_params=pltpu.CompilerParams(
            collective_id=0, has_side_effects=True, vmem_limit_bytes=40 * 1024 * 1024
        ),
    )(*kept)
    tile = min(512, model_width)
    wgrad_shape = jax.ShapeDtypeStruct((1, model_width, hidden), jnp.float32)
    token_grad, gate_wgrad, up_wgrad = pl.pallas_call(
        weight_grad_kernel,
        grid=(model_width // tile,),
        out_shape=(jax.ShapeDtypeStruct((token_count, model_width), bf16), wgrad_shape, wgrad_shape),
        in_specs=[in_vmem] * 5,
        out_specs=(
            pl.BlockSpec((token_count, tile), lambda i: (0, i)),
            pl.BlockSpec((1, tile, hidden), lambda i: (0, i, 0)),
            pl.BlockSpec((1, tile, hidden), lambda i: (0, i, 0)),
        ),
        compiler_params=pltpu.CompilerParams(vmem_limit_bytes=20 * 1024 * 1024),
    )(returned, block_rows, gate_rows, up_rows, selection)
    return (token_grad, gate_wgrad, up_wgrad)


def solution(mesh):
    placed = (
        P(("expert", "shard"), None),
        P(("expert", "shard"), None),
        P("expert", None, "shard"),
        P("expert", None, "shard"),
        P("expert", None, "shard"),
        P("expert", None, "shard"),
        P("expert", None, "shard"),
    )
    small = mesh.shape["shard"] == 8 and mesh.shape["expert"] == 4
    return jax.shard_map(
        on_device if small else on_device_general,
        mesh=mesh,
        in_specs=placed,
        out_specs=(
            P(("expert", "shard"), None),
            P("expert", None, "shard"),
            P("expert", None, "shard"),
        ),
        check_vma=False,
    )
```

```python
import functools
import jax
import jax.numpy as jnp
from jax import lax
from jax.experimental import pallas as pl
from jax.experimental.pallas import tpu as pltpu
from jax.sharding import PartitionSpec as P

MESH = pl.DeviceIdType.MESH
UNITS = 4
GATHERS = 3
SUMS = 8
AHEAD = 3
STEPS = 20
ORDER = (
    ("multiply", 0, 1),
    ("pair_sum", 1, 1),
    ("token_spread", 4, 1),
    ("near_sum", 3, 1),
    ("own_sum", 5, 1),
    ("spread", 7, 2),
    ("forward", 9, 2),
    ("token_pair", 12, 1),
    ("far", 11, 2),
    ("gathered", 13, 2),
    ("token_end", 16, 1),
)


def swiglu_grads(gate_values, up_values, hidden_cotangent):
    gate_float = gate_values.astype(jnp.float32)
    up_float = up_values.astype(jnp.float32)
    cotangent = hidden_cotangent.astype(jnp.float32)
    sigmoid_gate = jax.nn.sigmoid(gate_float)
    gate_grad = (
        cotangent * up_float * sigmoid_gate * (1.0 + gate_float * (1.0 - sigmoid_gate))
    ).astype(jnp.bfloat16)
    up_grad = (cotangent * gate_float * sigmoid_gate).astype(jnp.bfloat16)
    return (gate_grad, up_grad)


def slot_table(expert_ids, groups, capacity):
    token_count = expert_ids.shape[0]
    choices_per = expert_ids.shape[1]
    labels = lax.broadcasted_iota(jnp.int32, (1, 1, groups), 2)
    one_hot = (expert_ids[:, :, None] == labels).astype(jnp.int32)
    flat_hits = one_hot.reshape(token_count * choices_per, groups)
    earlier = jnp.cumsum(flat_hits, axis=0) - flat_hits
    slot_index = jnp.sum(flat_hits * earlier, axis=1).reshape(token_count, choices_per)
    slot_labels = lax.broadcasted_iota(jnp.int32, (1, 1, 1, capacity), 3)
    slot_hits = one_hot[:, :, :, None] * (slot_index[:, :, None, None] == slot_labels).astype(
        jnp.int32
    )
    selection = jnp.sum(slot_hits, axis=1).reshape(token_count, groups * capacity)
    return selection.astype(jnp.bfloat16)


def rows_inner(left_rows, right_rows):
    return lax.dot_general(
        left_rows, right_rows, (((0,), (0,)), ((), ())), preferred_element_type=jnp.float32
    )


def times_transposed(left_rows, weights):
    return lax.dot_general(
        left_rows, weights, (((1,), (1,)), ((), ())), preferred_element_type=jnp.float32
    )


def on_device_general(tokens, expert_ids, weight_gate, weight_up, gate_pre, up_pre, hidden_grad):
    groups = lax.axis_size("expert")
    shards = lax.axis_size("shard")
    model_width = tokens.shape[1]
    capacity = gate_pre.shape[1] // (groups * shards)
    selection = slot_table(expert_ids, groups, capacity)
    outgoing = rows_inner(selection, tokens).astype(jnp.bfloat16)
    gate_grad, up_grad = swiglu_grads(gate_pre[0], up_pre[0], hidden_grad[0])
    gate_matrix = weight_gate[0]
    up_matrix = weight_up[0]
    arrived = lax.all_to_all(
        outgoing.reshape(groups, capacity, model_width),
        "expert",
        split_axis=0,
        concat_axis=0,
        tiled=True,
    )
    block_rows = lax.all_gather(
        arrived.reshape(groups * capacity, model_width), "shard", axis=0, tiled=True
    )
    gate_rows = gate_grad
    up_rows = up_grad
    gate_wgrad = rows_inner(block_rows, gate_rows)
    up_wgrad = rows_inner(block_rows, up_rows)
    gate_rows = gate_grad
    up_rows = up_grad
    summed = lax.psum_scatter(
        (times_transposed(gate_rows, gate_matrix) + times_transposed(up_rows, up_matrix)).astype(
            jnp.bfloat16
        ),
        "shard",
        scatter_dimension=0,
        tiled=True,
    )
    outbound = summed.reshape(groups, capacity, model_width)
    returned = lax.all_to_all(outbound, "expert", split_axis=0, concat_axis=0, tiled=True)
    returned = returned.reshape(groups * capacity, model_width)
    token_grad = times_transposed(selection, returned.T).astype(jnp.bfloat16)
    return (token_grad, gate_wgrad[None], up_wgrad[None])


def slot_choice(expert_ids, groups, capacity):
    token_count = expert_ids.shape[1]
    lines = lax.broadcasted_iota(jnp.int32, (groups * capacity, token_count), 0)
    expert, slot = lines // capacity, lines % capacity
    named = jnp.logical_or(expert_ids[0:1, :] == expert, expert_ids[1:2, :] == expert)
    hits = jnp.where(named, 1.0, 0.0)
    above = lax.broadcasted_iota(jnp.int32, (token_count, token_count), 0)
    below = lax.broadcasted_iota(jnp.int32, (token_count, token_count), 1)
    before = jnp.where(above < below, 1.0, 0.0)
    earlier = jnp.dot(hits, before, preferred_element_type=jnp.float32)
    chosen = jnp.logical_and(named, earlier == slot.astype(jnp.float32))
    return jnp.where(chosen, 1.0, 0.0).astype(jnp.bfloat16)


def exchange_kernel(
    groups, capacity, expert_ids, tokens, weight_gate, weight_up, gate_pre, up_pre, hidden_grad,
    returned, block, gate_rows, up_rows, selection,
    choices, token_buf, outgoing, near_choices, near_tokens, near_outgoing, weights, pre, partial, from_core, total, from_diag,
    from_near, leaving, load_sem, send_sem, gather_sem, token_sem, sum_sem, return_sem,
):
    e = lax.axis_index("expert")
    q = lax.axis_index("shard")
    core, x, y = q % 2, (q // 2) % 2, q // 4
    sib = q + 1 - 2 * core
    xn = q + 2 - 4 * x
    yn = q + 4 - 8 * y
    dg = xn + 4 - 8 * y
    rows = groups * capacity
    half = rows // 2
    slots = gate_rows.shape[0]
    wide = block.shape[1] // UNITS
    slim = total.shape[2]
    tail = near_tokens.shape[2]
    late = slice(GATHERS * wide, GATHERS * wide + tail)
    peers = (q, xn, yn, dg)

    def columns(c, width):
        return pl.ds(pl.multiple_of(c * width, width), width)

    def span(start, size):
        return pl.ds(pl.multiple_of(start, size), size)

    def held(c, start, size):
        return block.at[span(start, size), columns(c, wide)]

    def chip_rows(c, device, low, size):
        return total.at[c, span(device // 2 * rows + low, size), :]

    def other(k):
        return (e + k) % groups

    def wait(place, sem):
        pltpu.make_async_copy(place, place, sem).wait()

    def target(k):
        if k < 3:
            return (other(k + 1), q)
        if k >= 18:
            return (other(k - 17), q)
        if k in (3, 7, 12, 14, 16):
            return (e, xn)
        if k in (4, 6, 13, 15, 17):
            return (e, yn)
        return (e, sib)

    def copy(k, c):
        if k < 3:
            source = outgoing.at[other(k + 1), :, columns(c, wide)]
            to = held(c, q * rows + e * capacity, capacity)
        elif k < 6:
            source = to = held(c, q * rows, rows)
        elif k == 6:
            source = to = held(c, xn * rows, half)
        elif k == 7:
            source = to = held(c, yn * rows + half, half)
        elif k < 11:
            source = to = held(c, (xn, yn, dg)[k - 8] * rows, rows)
        elif k == 11:
            source, to = partial.at[c, 1 - core], from_core.at[c]
        elif k == 12:
            source, to = chip_rows(c, dg, 0, half), from_diag.at[c, 0]
        elif k == 13:
            source, to = chip_rows(c, dg, half, half), from_diag.at[c, 1]
        elif k == 14:
            source, to = chip_rows(c, xn, 0, half), from_near.at[c, 0, 0]
        elif k == 15:
            source, to = chip_rows(c, yn, half, half), from_near.at[c, 1, 1]
        elif k == 16:
            source, to = chip_rows(c, xn, half, half), from_near.at[c, 0, 1]
        elif k == 17:
            source, to = chip_rows(c, yn, 0, half), from_near.at[c, 1, 0]
        else:
            source = leaving.at[c, span(other(k - 17) * capacity, capacity), :]
            to = returned.at[span(e * capacity, capacity), columns(c, slim)]
        if k < 11:
            recv = gather_sem.at[c, (0, 0, 0, 1, 2, 4, 3, 3, 4, 4, 4)[k]]
        elif k < 18:
            recv = sum_sem.at[c, (0, 1, 1, 2, 2, 2, 2)[k - 11]]
        else:
            recv = return_sem.at[0]
        return pltpu.make_async_remote_copy(
            src_ref=source, dst_ref=to, send_sem=send_sem.at[0], recv_sem=recv,
            device_id=target(k), device_id_type=MESH,
        )

    def remote(source, to, recv, device, sent):
        return pltpu.make_async_remote_copy(
            src_ref=source, dst_ref=to, send_sem=send_sem.at[sent], recv_sem=token_sem.at[recv],
            device_id=device, device_id_type=MESH,
        )

    def announce():
        for i, peer in enumerate(peers[1:]):
            remote(choices, near_choices.at[i], 0, (e, peer), 1).start()
            remote(token_buf.at[:, late], near_tokens.at[i], 1, (e, peer), 2).start()

    def late_rows(peer, start, size):
        return block.at[span(peer * rows + start, size), late]

    def token_spread(c):
        wait(near_choices, token_sem.at[0])
        wait(near_tokens, token_sem.at[1])
        for i in range(3):
            picked = jnp.dot(
                slot_choice(near_choices[i], groups, capacity), near_tokens[i],
                preferred_element_type=jnp.float32,
            ).astype(jnp.bfloat16)
            for group in range(groups):
                near_outgoing[i, group] = picked[group * capacity : (group + 1) * capacity]
        for k in (1, 0, 2):
            for i, peer in enumerate(peers):
                if i == 0:
                    source = outgoing.at[other(k + 1), :, late]
                else:
                    source = near_outgoing.at[i - 1, other(k + 1)]
                to = late_rows(peer, e * capacity, capacity)
                remote(source, to, 2, (other(k + 1), q), 3).start()
        for i, peer in enumerate(peers[1:]):
            block[span(peer * rows + e * capacity, capacity), late] = near_outgoing[i, e]

    def token_pair(c):
        wait(block.at[pl.ds(0, 12 * capacity), late], token_sem.at[2])
        for peer in peers:
            place = late_rows(peer, 0, rows)
            remote(place, place, 3, (e, sib), 3).start()

    def token_end(c):
        wait(block.at[pl.ds(0, 4 * rows), late], token_sem.at[3])

    def weight_loads(c):
        for i, source in enumerate((weight_gate, weight_up)):
            pltpu.make_async_copy(
                source.at[0, columns(c, slim), :], weights.at[c, i], load_sem.at[c]
            ).start()

    token_load = pltpu.make_async_copy(tokens, token_buf, load_sem.at[SUMS])
    token_load.start()
    choice_load = pltpu.make_async_copy(expert_ids, choices, load_sem.at[SUMS + 2])
    choice_load.start()
    for i, source in enumerate((gate_pre, up_pre, hidden_grad)):
        pltpu.make_async_copy(source.at[0], pre.at[i], load_sem.at[SUMS + 1]).start()
    for c in range(AHEAD):
        weight_loads(c)

    barrier = pltpu.get_barrier_semaphore()
    for device in [(other(k), q) for k in (1, 2, 3)] + [(e, peer) for peer in (sib, xn, yn, dg)]:
        pl.semaphore_signal(barrier, inc=1, device_id=device, device_id_type=MESH)
    choice_load.wait()
    selection[...] = slot_choice(choices[...], groups, capacity)
    token_load.wait()
    for c in range(UNITS):
        here = slice(c * wide, (c + 1) * wide)
        picked = jnp.dot(
            selection[...], token_buf[:, here], preferred_element_type=jnp.float32
        ).astype(jnp.bfloat16)
        for group in range(groups):
            outgoing[group, :, here] = picked[group * capacity : (group + 1) * capacity]

    @pl.loop(0, UNITS)
    def _(c):
        here = columns(c, wide)
        block[span(q * rows + e * capacity, capacity), here] = outgoing[e, :, here]

    wait(pre, load_sem.at[SUMS + 1])
    step_rows = 32

    @pl.loop(0, slots // step_rows)
    def _(i):
        here = span(i * step_rows, step_rows)
        gate_grad, up_grad = swiglu_grads(pre[0, here, :], pre[1, here, :], pre[2, here, :])
        gate_rows[here, :] = gate_grad
        up_rows[here, :] = up_grad

    def multiply(c):
        @pl.when(c < SUMS - AHEAD)
        def _():
            weight_loads(c + AHEAD)

        wait(weights.at[c], load_sem.at[c])
        term = times_transposed(gate_rows[...], weights[c, 0]) + times_transposed(
            up_rows[...], weights[c, 1]
        )
        term = term.astype(jnp.bfloat16)
        for chip in range(slots // (2 * rows)):
            for side in range(2):
                low = (2 * chip + side) * rows
                partial[c, side, chip * rows : (chip + 1) * rows, :] = term[low : low + rows]

        @pl.when(c == 0)
        def _():
            pl.semaphore_wait(barrier, 7)
            announce()

            @pl.loop(0, GATHERS)
            def _(i):
                for k in (1, 0, 2):
                    copy(k, i).start()

        copy(11, c).start()

    def spread(c):
        wait(held(c, 0, 3 * capacity), gather_sem.at[c, 0])
        for k in (3, 4, 5):
            copy(k, c).start()

    def forward(c):
        wait(held(c, 0, rows), gather_sem.at[c, 1])
        copy(6, c).start()
        copy(8, c).start()
        wait(held(c, 0, rows), gather_sem.at[c, 2])
        copy(7, c).start()
        copy(9, c).start()

    def far(c):
        wait(held(c, 0, rows), gather_sem.at[c, 3])
        copy(10, c).start()

    def gathered(c):
        wait(held(c, 0, 4 * rows), gather_sem.at[c, 4])

    def pair_sum(c):
        wait(from_core.at[c], sum_sem.at[c, 0])
        both = partial[c, core].astype(jnp.float32) + from_core[c].astype(jnp.float32)
        total[c] = both.astype(jnp.bfloat16)
        for k in (12, 13, 14, 15):
            copy(k, c).start()

    def near_sum(c):
        wait(from_diag.at[c], sum_sem.at[c, 1])
        for side, device, low in ((0, yn, 0), (1, xn, half)):
            place = span(device // 2 * rows + low, half)
            added = total[c, place, :].astype(jnp.float32) + from_diag[c, side].astype(jnp.float32)
            total[c, place, :] = added.astype(jnp.bfloat16)
            copy(17 if side == 0 else 16, c).start()

    def own_sum(c):
        wait(from_near.at[c], sum_sem.at[c, 2])
        for low in range(2):
            place = span(q // 2 * rows + low * half, half)
            added = total[c, place, :].astype(jnp.float32)
            added = added + from_near[c, 0, low].astype(jnp.float32)
            added = added + from_near[c, 1, low].astype(jnp.float32)
            leaving[c, low * half : (low + 1) * half, :] = added.astype(jnp.bfloat16)
        mine = span(e * capacity, capacity)
        returned[mine, columns(c, slim)] = leaving[c, mine, :]
        for k in (19, 18, 20):
            copy(k, c).start()

    stages = dict(
        multiply=(multiply, SUMS), pair_sum=(pair_sum, SUMS), near_sum=(near_sum, SUMS),
        own_sum=(own_sum, SUMS), spread=(spread, GATHERS), forward=(forward, GATHERS),
        far=(far, GATHERS), gathered=(gathered, GATHERS), token_spread=(token_spread, 1),
        token_pair=(token_pair, 1), token_end=(token_end, 1),
    )

    @pl.loop(0, STEPS)
    def _(step):
        for name, first, every in ORDER:
            stage, count = stages[name]
            c = (step - first) // every
            ready = jnp.logical_and(step >= first, step < first + every * count)
            if every > 1:
                ready = jnp.logical_and(ready, (step - first) % every == 0)

            @pl.when(ready)
            def _():
                stage(c)

    wait(returned.at[pl.ds(0, 3 * capacity), :], return_sem.at[0])
    sent = (3 * capacity + 6 * rows + 2 * half) * GATHERS * wide
    sent = sent + (3 * capacity + 6 * half + slots // 2) * SUMS * slim
    wait(weight_gate.at[0, pl.ds(0, sent // weight_gate.shape[2]), :], send_sem.at[0])
    wait(near_choices, send_sem.at[1])
    wait(near_tokens, send_sem.at[2])
    wait(block.at[pl.ds(0, 12 * capacity + 4 * rows), late], send_sem.at[3])


def weight_grad_kernel(
    returned, block_rows, gate_rows, up_rows, selection, token_grad, gate_wgrad, up_wgrad,
):
    tile = gate_wgrad.shape[1]
    here = pl.ds(pl.multiple_of(pl.program_id(0) * tile, tile), tile)
    left = block_rows[:, here]
    gate_wgrad[0] = rows_inner(left, gate_rows[...])
    up_wgrad[0] = rows_inner(left, up_rows[...])
    token_grad[...] = rows_inner(selection[...], returned[:, here]).astype(jnp.bfloat16)


def on_device(tokens, expert_ids, weight_gate, weight_up, gate_pre, up_pre, hidden_grad):
    groups = lax.axis_size("expert")
    shards = lax.axis_size("shard")
    token_count, model_width = tokens.shape
    slots, hidden = gate_pre.shape[1:]
    capacity = slots // (groups * shards)
    rows = groups * capacity
    slim = model_width // SUMS
    tail = model_width // UNITS * (UNITS - GATHERS)
    bf16 = jnp.bfloat16
    kept = [
        pltpu.with_memory_space_constraint(array, pltpu.HBM)
        for array in (expert_ids.T, tokens, weight_gate, weight_up, gate_pre, up_pre, hidden_grad)
    ]
    in_vmem = pl.BlockSpec(memory_space=pltpu.VMEM)
    in_hbm = pl.BlockSpec(memory_space=pltpu.HBM)
    returned, block_rows, gate_rows, up_rows, selection = pl.pallas_call(
        functools.partial(exchange_kernel, groups, capacity),
        out_shape=(
            jax.ShapeDtypeStruct((rows, model_width), bf16),
            jax.ShapeDtypeStruct((slots, model_width), bf16),
            jax.ShapeDtypeStruct((slots, hidden), bf16),
            jax.ShapeDtypeStruct((slots, hidden), bf16),
            jax.ShapeDtypeStruct((rows, token_count), bf16),
        ),
        in_specs=[in_hbm] * 7,
        out_specs=(in_vmem,) * 5,
        scratch_shapes=[
            pltpu.VMEM(expert_ids.shape[::-1], expert_ids.dtype),
            pltpu.VMEM((token_count, model_width), bf16),
            pltpu.VMEM((groups, capacity, model_width), bf16),
            pltpu.VMEM((3, *expert_ids.shape[::-1]), expert_ids.dtype),
            pltpu.VMEM((3, token_count, tail), bf16),
            pltpu.VMEM((3, groups, capacity, tail), bf16),
            pltpu.VMEM((SUMS, 2, slim, hidden), bf16),
            pltpu.VMEM((3, slots, hidden), bf16),
            pltpu.VMEM((SUMS, 2, slots // 2, slim), bf16),
            pltpu.VMEM((SUMS, slots // 2, slim), bf16),
            pltpu.VMEM((SUMS, slots // 2, slim), bf16),
            pltpu.VMEM((SUMS, 2, rows // 2, slim), bf16),
            pltpu.VMEM((SUMS, 2, 2, rows // 2, slim), bf16),
            pltpu.VMEM((SUMS, rows, slim), bf16),
            pltpu.SemaphoreType.DMA((SUMS + 3,)),
            pltpu.SemaphoreType.DMA((4,)),
            pltpu.SemaphoreType.DMA((GATHERS, 5)),
            pltpu.SemaphoreType.DMA((4,)),
            pltpu.SemaphoreType.DMA((SUMS, 3)),
            pltpu.SemaphoreType.DMA((1,)),
        ],
        compiler_params=pltpu.CompilerParams(
            collective_id=0, has_side_effects=True, vmem_limit_bytes=40 * 1024 * 1024
        ),
    )(*kept)
    tile = min(512, model_width)
    wgrad_shape = jax.ShapeDtypeStruct((1, model_width, hidden), jnp.float32)
    token_grad, gate_wgrad, up_wgrad = pl.pallas_call(
        weight_grad_kernel,
        grid=(model_width // tile,),
        out_shape=(jax.ShapeDtypeStruct((token_count, model_width), bf16), wgrad_shape, wgrad_shape),
        in_specs=[in_vmem] * 5,
        out_specs=(
            pl.BlockSpec((token_count, tile), lambda i: (0, i)),
            pl.BlockSpec((1, tile, hidden), lambda i: (0, i, 0)),
            pl.BlockSpec((1, tile, hidden), lambda i: (0, i, 0)),
        ),
        compiler_params=pltpu.CompilerParams(vmem_limit_bytes=20 * 1024 * 1024),
    )(returned, block_rows, gate_rows, up_rows, selection)
    return (token_grad, gate_wgrad, up_wgrad)


def solution(mesh):
    placed = (
        P(("expert", "shard"), None),
        P(("expert", "shard"), None),
        P("expert", None, "shard"),
        P("expert", None, "shard"),
        P("expert", None, "shard"),
        P("expert", None, "shard"),
        P("expert", None, "shard"),
    )
    small = mesh.shape["shard"] == 8 and mesh.shape["expert"] == 4
    return jax.shard_map(
        on_device if small else on_device_general,
        mesh=mesh,
        in_specs=placed,
        out_specs=(
            P(("expert", "shard"), None),
            P("expert", None, "shard"),
            P("expert", None, "shard"),
        ),
        check_vma=False,
    )
```

```python
import functools
import jax
import jax.numpy as jnp
from jax import lax
from jax.experimental import pallas as pl
from jax.experimental.pallas import tpu as pltpu
from jax.sharding import PartitionSpec as P

MESH = pl.DeviceIdType.MESH
UNITS = 4
GATHERS = 3
SUMS = 8
AHEAD = 2
STEPS = 18
ORDER = (
    ("multiply", 0, 1),
    ("pair_sum", 1, 1),
    ("token_spread", 3, 1),
    ("near_sum", 3, 1),
    ("own_sum", 5, 1),
    ("spread", 8, 1),
    ("forward", 10, 1),
    ("token_pair", 13, 1),
    ("far", 12, 1),
    ("gathered", 14, 1),
    ("token_end", 16, 1),
)


def tiles_of(quarter):
    return (quarter // 2, quarter, quarter, quarter, quarter // 2)


def swiglu_grads(gate_values, up_values, hidden_cotangent):
    gate_float = gate_values.astype(jnp.float32)
    up_float = up_values.astype(jnp.float32)
    cotangent = hidden_cotangent.astype(jnp.float32)
    sigmoid_gate = jax.nn.sigmoid(gate_float)
    gate_grad = (
        cotangent * up_float * sigmoid_gate * (1.0 + gate_float * (1.0 - sigmoid_gate))
    ).astype(jnp.bfloat16)
    up_grad = (cotangent * gate_float * sigmoid_gate).astype(jnp.bfloat16)
    return (gate_grad, up_grad)


def slot_table(expert_ids, groups, capacity):
    token_count = expert_ids.shape[0]
    choices_per = expert_ids.shape[1]
    labels = lax.broadcasted_iota(jnp.int32, (1, 1, groups), 2)
    one_hot = (expert_ids[:, :, None] == labels).astype(jnp.int32)
    flat_hits = one_hot.reshape(token_count * choices_per, groups)
    earlier = jnp.cumsum(flat_hits, axis=0) - flat_hits
    slot_index = jnp.sum(flat_hits * earlier, axis=1).reshape(token_count, choices_per)
    slot_labels = lax.broadcasted_iota(jnp.int32, (1, 1, 1, capacity), 3)
    slot_hits = one_hot[:, :, :, None] * (slot_index[:, :, None, None] == slot_labels).astype(
        jnp.int32
    )
    selection = jnp.sum(slot_hits, axis=1).reshape(token_count, groups * capacity)
    return selection.astype(jnp.bfloat16)


def rows_inner(left_rows, right_rows):
    return lax.dot_general(
        left_rows, right_rows, (((0,), (0,)), ((), ())), preferred_element_type=jnp.float32
    )


def times_transposed(left_rows, weights):
    return lax.dot_general(
        left_rows, weights, (((1,), (1,)), ((), ())), preferred_element_type=jnp.float32
    )


def on_device_general(tokens, expert_ids, weight_gate, weight_up, gate_pre, up_pre, hidden_grad):
    groups = lax.axis_size("expert")
    shards = lax.axis_size("shard")
    model_width = tokens.shape[1]
    capacity = gate_pre.shape[1] // (groups * shards)
    selection = slot_table(expert_ids, groups, capacity)
    outgoing = rows_inner(selection, tokens).astype(jnp.bfloat16)
    gate_grad, up_grad = swiglu_grads(gate_pre[0], up_pre[0], hidden_grad[0])
    gate_matrix = weight_gate[0]
    up_matrix = weight_up[0]
    arrived = lax.all_to_all(
        outgoing.reshape(groups, capacity, model_width),
        "expert",
        split_axis=0,
        concat_axis=0,
        tiled=True,
    )
    block_rows = lax.all_gather(
        arrived.reshape(groups * capacity, model_width), "shard", axis=0, tiled=True
    )
    gate_rows = gate_grad
    up_rows = up_grad
    gate_wgrad = rows_inner(block_rows, gate_rows)
    up_wgrad = rows_inner(block_rows, up_rows)
    gate_rows = gate_grad
    up_rows = up_grad
    summed = lax.psum_scatter(
        (times_transposed(gate_rows, gate_matrix) + times_transposed(up_rows, up_matrix)).astype(
            jnp.bfloat16
        ),
        "shard",
        scatter_dimension=0,
        tiled=True,
    )
    outbound = summed.reshape(groups, capacity, model_width)
    returned = lax.all_to_all(outbound, "expert", split_axis=0, concat_axis=0, tiled=True)
    returned = returned.reshape(groups * capacity, model_width)
    token_grad = times_transposed(selection, returned.T).astype(jnp.bfloat16)
    return (token_grad, gate_wgrad[None], up_wgrad[None])


def slot_choice(expert_ids, groups, capacity):
    token_count = expert_ids.shape[1]
    lines = lax.broadcasted_iota(jnp.int32, (groups * capacity, token_count), 0)
    expert, slot = lines // capacity, lines % capacity
    named = jnp.logical_or(expert_ids[0:1, :] == expert, expert_ids[1:2, :] == expert)
    hits = jnp.where(named, 1.0, 0.0)
    above = lax.broadcasted_iota(jnp.int32, (token_count, token_count), 0)
    below = lax.broadcasted_iota(jnp.int32, (token_count, token_count), 1)
    before = jnp.where(above < below, 1.0, 0.0)
    earlier = jnp.dot(hits, before, preferred_element_type=jnp.float32)
    chosen = jnp.logical_and(named, earlier == slot.astype(jnp.float32))
    return jnp.where(chosen, 1.0, 0.0).astype(jnp.bfloat16)


def exchange_kernel(
    groups, capacity, expert_ids, tokens, weight_gate, weight_up, gate_pre, up_pre, hidden_grad,
    returned, block, gate_rows, up_rows, selection,
    choices, token_buf, outgoing, near_choices, near_tokens, near_outgoing, weights, pre, partial, from_core, total, from_diag,
    from_near, leaving, load_sem, send_sem, gather_sem, token_sem, sum_sem, return_sem,
):
    e = lax.axis_index("expert")
    q = lax.axis_index("shard")
    core, x, y = q % 2, (q // 2) % 2, q // 4
    sib = q + 1 - 2 * core
    xn = q + 2 - 4 * x
    yn = q + 4 - 8 * y
    dg = xn + 4 - 8 * y
    rows = groups * capacity
    half = rows // 2
    slots = gate_rows.shape[0]
    wide = block.shape[1] // UNITS
    slim = total.shape[2]
    tail = near_tokens.shape[2]
    late = slice(GATHERS * wide, GATHERS * wide + tail)
    peers = (q, xn, yn, dg)

    def columns(c, width):
        return pl.ds(pl.multiple_of(c * width, width), width)

    def span(start, size):
        return pl.ds(pl.multiple_of(start, size), size)

    def held(c, start, size):
        return block.at[span(start, size), columns(c, wide)]

    def chip_rows(c, device, low, size):
        return total.at[c, span(device // 2 * rows + low, size), :]

    def other(k):
        return (e + k) % groups

    def wait(place, sem):
        pltpu.make_async_copy(place, place, sem).wait()

    def target(k):
        if k < 3:
            return (other(k + 1), q)
        if k >= 18:
            return (other(k - 17), q)
        if k in (3, 7, 12, 14, 16):
            return (e, xn)
        if k in (4, 6, 13, 15, 17):
            return (e, yn)
        return (e, sib)

    def copy(k, c, piece=None):
        if k < 3:
            source = outgoing.at[other(k + 1), :, columns(c, wide)]
            to = held(c, q * rows + e * capacity, capacity)
        elif k < 6:
            source = to = held(c, q * rows, rows)
            if piece is not None:
                source = to = held(c, q * rows + other(piece) * capacity, capacity)
        elif k == 6:
            source = to = held(c, xn * rows, half)
        elif k == 7:
            source = to = held(c, yn * rows + half, half)
        elif k < 11:
            source = to = held(c, (xn, yn, dg)[k - 8] * rows, rows)
        elif k == 11:
            source, to = partial.at[c, 1 - core], from_core.at[c]
        elif k == 12:
            source, to = chip_rows(c, dg, 0, half), from_diag.at[c, 0]
        elif k == 13:
            source, to = chip_rows(c, dg, half, half), from_diag.at[c, 1]
        elif k == 14:
            source, to = chip_rows(c, xn, 0, half), from_near.at[c, 0, 0]
        elif k == 15:
            source, to = chip_rows(c, yn, half, half), from_near.at[c, 1, 1]
        elif k == 16:
            source, to = chip_rows(c, xn, half, half), from_near.at[c, 0, 1]
        elif k == 17:
            source, to = chip_rows(c, yn, 0, half), from_near.at[c, 1, 0]
        else:
            source = leaving.at[c, span(other(k - 17) * capacity, capacity), :]
            to = returned.at[span(e * capacity, capacity), columns(c, slim)]
        if k < 11:
            recv = gather_sem.at[c, (0, 0, 0, 1, 2, 4, 3, 3, 4, 4, 4)[k]]
        elif k < 18:
            recv = sum_sem.at[c, (0, 1, 1, 2, 2, 2, 2)[k - 11]]
        else:
            recv = return_sem.at[0]
        return pltpu.make_async_remote_copy(
            src_ref=source, dst_ref=to, send_sem=send_sem.at[0], recv_sem=recv,
            device_id=target(k), device_id_type=MESH,
        )

    def remote(source, to, recv, device, sent):
        return pltpu.make_async_remote_copy(
            src_ref=source, dst_ref=to, send_sem=send_sem.at[sent], recv_sem=token_sem.at[recv],
            device_id=device, device_id_type=MESH,
        )

    def announce():
        for i, peer in enumerate(peers[1:]):
            remote(choices, near_choices.at[i], 0, (e, peer), 1).start()
            remote(token_buf.at[:, late], near_tokens.at[i], 1, (e, peer), 2).start()

    def late_rows(peer, start, size):
        return block.at[span(peer * rows + start, size), late]

    def token_spread(c):
        wait(near_choices, token_sem.at[0])
        wait(near_tokens, token_sem.at[1])
        for i in range(3):
            picked = jnp.dot(
                slot_choice(near_choices[i], groups, capacity), near_tokens[i],
                preferred_element_type=jnp.float32,
            ).astype(jnp.bfloat16)
            for group in range(groups):
                near_outgoing[i, group] = picked[group * capacity : (group + 1) * capacity]
        for k in (1, 0, 2):
            for i, peer in enumerate(peers):
                if i == 0:
                    source = outgoing.at[other(k + 1), :, late]
                else:
                    source = near_outgoing.at[i - 1, other(k + 1)]
                to = late_rows(peer, e * capacity, capacity)
                remote(source, to, 2, (other(k + 1), q), 3).start()
        for i, peer in enumerate(peers[1:]):
            block[span(peer * rows + e * capacity, capacity), late] = near_outgoing[i, e]

    def token_pair(c):
        wait(block.at[pl.ds(0, 12 * capacity), late], token_sem.at[2])
        for peer in peers:
            place = late_rows(peer, 0, rows)
            remote(place, place, 3, (e, sib), 3).start()

    def token_end(c):
        wait(block.at[pl.ds(0, 4 * rows), late], token_sem.at[3])

    def weight_loads(c):
        for i, source in enumerate((weight_gate, weight_up)):
            pltpu.make_async_copy(
                source.at[0, columns(c, slim), :], weights.at[c, i], load_sem.at[c]
            ).start()

    token_load = pltpu.make_async_copy(tokens, token_buf, load_sem.at[SUMS])
    token_load.start()
    choice_load = pltpu.make_async_copy(expert_ids, choices, load_sem.at[SUMS + 2])
    choice_load.start()
    for i, source in enumerate((gate_pre, up_pre, hidden_grad)):
        pltpu.make_async_copy(source.at[0], pre.at[i], load_sem.at[SUMS + 1]).start()
    for c in range(AHEAD):
        weight_loads(c)

    barrier = pltpu.get_barrier_semaphore()
    for device in [(other(k), q) for k in (1, 2, 3)] + [(e, peer) for peer in (sib, xn, yn, dg)]:
        pl.semaphore_signal(barrier, inc=1, device_id=device, device_id_type=MESH)
    choice_load.wait()
    selection[...] = slot_choice(choices[...], groups, capacity)
    token_load.wait()
    for c in range(UNITS):
        here = slice(c * wide, (c + 1) * wide)
        picked = jnp.dot(
            selection[...], token_buf[:, here], preferred_element_type=jnp.float32
        ).astype(jnp.bfloat16)
        for group in range(groups):
            outgoing[group, :, here] = picked[group * capacity : (group + 1) * capacity]

    @pl.loop(0, UNITS)
    def _(c):
        here = columns(c, wide)
        block[span(q * rows + e * capacity, capacity), here] = outgoing[e, :, here]

    wait(pre, load_sem.at[SUMS + 1])
    step_rows = 32

    @pl.loop(0, slots // step_rows)
    def _(i):
        here = span(i * step_rows, step_rows)
        gate_grad, up_grad = swiglu_grads(pre[0, here, :], pre[1, here, :], pre[2, here, :])
        gate_rows[here, :] = gate_grad
        up_rows[here, :] = up_grad

    def products(c, low, size):
        term = times_transposed(gate_rows[low : low + size, :], weights[c, 0])
        term = term + times_transposed(up_rows[low : low + size, :], weights[c, 1])
        term = term.astype(jnp.bfloat16)
        for piece in range(size // rows):
            chip, side = divmod(low // rows + piece, 2)
            partial[c, side, chip * rows : (chip + 1) * rows, :] = term[
                piece * rows : (piece + 1) * rows
            ]

    def multiply(c):
        @pl.when(c < SUMS - AHEAD)
        def _():
            weight_loads(c + AHEAD)

        wait(weights.at[c], load_sem.at[c])
        products(c, 0, slots)
        copy(11, c).start()

    def spread(c):
        wait(held(c, 0, 3 * capacity), gather_sem.at[c, 0])
        for k in (3, 4):
            for piece in (1, 2, 3):
                copy(k, c, piece).start()
        copy(5, c).start()

    def forward(c):
        wait(held(c, 0, rows), gather_sem.at[c, 1])
        copy(6, c).start()
        copy(8, c).start()
        wait(held(c, 0, rows), gather_sem.at[c, 2])
        copy(7, c).start()
        copy(9, c).start()

    def far(c):
        wait(held(c, 0, rows), gather_sem.at[c, 3])
        copy(10, c).start()

    def gathered(c):
        wait(held(c, 0, 4 * rows), gather_sem.at[c, 4])

    def pair_sum(c):
        wait(from_core.at[c], sum_sem.at[c, 0])
        both = partial[c, core].astype(jnp.float32) + from_core[c].astype(jnp.float32)
        total[c] = both.astype(jnp.bfloat16)
        for k in (12, 13, 14, 15):
            copy(k, c).start()

    def near_sum(c):
        wait(from_diag.at[c], sum_sem.at[c, 1])
        for side, device, low in ((0, yn, 0), (1, xn, half)):
            place = span(device // 2 * rows + low, half)
            added = total[c, place, :].astype(jnp.float32) + from_diag[c, side].astype(jnp.float32)
            total[c, place, :] = added.astype(jnp.bfloat16)
            copy(17 if side == 0 else 16, c).start()

    def own_sum(c):
        wait(from_near.at[c], sum_sem.at[c, 2])
        for low in range(2):
            place = span(q // 2 * rows + low * half, half)
            added = total[c, place, :].astype(jnp.float32)
            added = added + from_near[c, 0, low].astype(jnp.float32)
            added = added + from_near[c, 1, low].astype(jnp.float32)
            leaving[c, low * half : (low + 1) * half, :] = added.astype(jnp.bfloat16)
        mine = span(e * capacity, capacity)
        returned[mine, columns(c, slim)] = leaving[c, mine, :]
        for k in (19, 18, 20):
            copy(k, c).start()

    weight_loads(AHEAD)
    wait(weights.at[0], load_sem.at[0])
    products(0, 0, slots // 2)
    pl.semaphore_wait(barrier, 7)
    announce()

    @pl.loop(0, GATHERS)
    def _(c):
        for k in (1, 0, 2):
            copy(k, c).start()
        for k in (3, 4):
            copy(k, c, 0).start()

    products(0, slots // 2, slots // 2)
    copy(11, 0).start()
    stages = dict(
        multiply=(multiply, SUMS), pair_sum=(pair_sum, SUMS), near_sum=(near_sum, SUMS),
        own_sum=(own_sum, SUMS), spread=(spread, GATHERS), forward=(forward, GATHERS),
        far=(far, GATHERS), gathered=(gathered, GATHERS), token_spread=(token_spread, 1),
        token_pair=(token_pair, 1), token_end=(token_end, 1),
    )

    @pl.loop(1, STEPS)
    def _(step):
        for name, first, every in ORDER:
            stage, count = stages[name]
            c = (step - first) // every
            ready = jnp.logical_and(step >= first, step < first + every * count)
            if every > 1:
                ready = jnp.logical_and(ready, (step - first) % every == 0)

            @pl.when(ready)
            def _():
                stage(c)

    wait(returned.at[pl.ds(0, 3 * capacity), :], return_sem.at[0])
    sent = (3 * capacity + 6 * rows + 2 * half) * GATHERS * wide
    sent = sent + (3 * capacity + 6 * half + slots // 2) * SUMS * slim
    wait(weight_gate.at[0, pl.ds(0, sent // weight_gate.shape[2]), :], send_sem.at[0])
    wait(near_choices, send_sem.at[1])
    wait(near_tokens, send_sem.at[2])
    wait(block.at[pl.ds(0, 12 * capacity + 4 * rows), late], send_sem.at[3])


def weight_grad_kernel(
    returned, block_rows, gate_rows, up_rows, selection, token_grad, gate_wgrad, up_wgrad,
    staged, token_staged, store_sem, token_sem,
):
    quarter = block_rows.shape[1] // 4
    tiles = tiles_of(quarter)
    stores = []
    low = 0
    for i, tile in enumerate(tiles):
        here = slice(low, low + tile)
        for j, (grads, wgrad) in enumerate(((gate_rows, gate_wgrad), (up_rows, up_wgrad))):
            if i >= 2:
                stores[2 * i + j - 4].wait()
            place = staged.at[i % 2, j, pl.ds(0, tile), :]
            place[...] = rows_inner(block_rows[:, here], grads[...])
            stores.append(
                pltpu.make_async_copy(place, wgrad.at[0, pl.ds(low, tile), :], store_sem.at[i % 2, j])
            )
            stores[-1].start()
        if i == 1:
            token_staged[...] = rows_inner(selection[...], returned[...]).astype(jnp.bfloat16)
            token_store = pltpu.make_async_copy(token_staged, token_grad, token_sem.at[0])
            token_store.start()
        low += tile
    for store in stores[-4:]:
        store.wait()
    token_store.wait()


def on_device(tokens, expert_ids, weight_gate, weight_up, gate_pre, up_pre, hidden_grad):
    groups = lax.axis_size("expert")
    shards = lax.axis_size("shard")
    token_count, model_width = tokens.shape
    slots, hidden = gate_pre.shape[1:]
    capacity = slots // (groups * shards)
    rows = groups * capacity
    slim = model_width // SUMS
    tail = model_width // UNITS * (UNITS - GATHERS)
    bf16 = jnp.bfloat16
    kept = [
        pltpu.with_memory_space_constraint(array, pltpu.HBM)
        for array in (expert_ids.T, tokens, weight_gate, weight_up, gate_pre, up_pre, hidden_grad)
    ]
    in_vmem = pl.BlockSpec(memory_space=pltpu.VMEM)
    in_hbm = pl.BlockSpec(memory_space=pltpu.HBM)
    returned, block_rows, gate_rows, up_rows, selection = pl.pallas_call(
        functools.partial(exchange_kernel, groups, capacity),
        out_shape=(
            jax.ShapeDtypeStruct((rows, model_width), bf16),
            jax.ShapeDtypeStruct((slots, model_width), bf16),
            jax.ShapeDtypeStruct((slots, hidden), bf16),
            jax.ShapeDtypeStruct((slots, hidden), bf16),
            jax.ShapeDtypeStruct((rows, token_count), bf16),
        ),
        in_specs=[in_hbm] * 7,
        out_specs=(in_vmem,) * 5,
        scratch_shapes=[
            pltpu.VMEM(expert_ids.shape[::-1], expert_ids.dtype),
            pltpu.VMEM((token_count, model_width), bf16),
            pltpu.VMEM((groups, capacity, model_width), bf16),
            pltpu.VMEM((3, *expert_ids.shape[::-1]), expert_ids.dtype),
            pltpu.VMEM((3, token_count, tail), bf16),
            pltpu.VMEM((3, groups, capacity, tail), bf16),
            pltpu.VMEM((SUMS, 2, slim, hidden), bf16),
            pltpu.VMEM((3, slots, hidden), bf16),
            pltpu.VMEM((SUMS, 2, slots // 2, slim), bf16),
            pltpu.VMEM((SUMS, slots // 2, slim), bf16),
            pltpu.VMEM((SUMS, slots // 2, slim), bf16),
            pltpu.VMEM((SUMS, 2, rows // 2, slim), bf16),
            pltpu.VMEM((SUMS, 2, 2, rows // 2, slim), bf16),
            pltpu.VMEM((SUMS, rows, slim), bf16),
            pltpu.SemaphoreType.DMA((SUMS + 3,)),
            pltpu.SemaphoreType.DMA((4,)),
            pltpu.SemaphoreType.DMA((GATHERS, 5)),
            pltpu.SemaphoreType.DMA((4,)),
            pltpu.SemaphoreType.DMA((SUMS, 3)),
            pltpu.SemaphoreType.DMA((1,)),
        ],
        compiler_params=pltpu.CompilerParams(
            collective_id=0, has_side_effects=True, vmem_limit_bytes=40 * 1024 * 1024
        ),
    )(*kept)
    wgrad_shape = jax.ShapeDtypeStruct((1, model_width, hidden), jnp.float32)
    token_grad, gate_wgrad, up_wgrad = pl.pallas_call(
        weight_grad_kernel,
        out_shape=(jax.ShapeDtypeStruct((token_count, model_width), bf16), wgrad_shape, wgrad_shape),
        in_specs=[in_vmem] * 5,
        out_specs=(in_hbm,) * 3,
        scratch_shapes=[
            pltpu.VMEM((2, 2, model_width // 4, hidden), jnp.float32),
            pltpu.VMEM((token_count, model_width), bf16),
            pltpu.SemaphoreType.DMA((2, 2)),
            pltpu.SemaphoreType.DMA((1,)),
        ],
        compiler_params=pltpu.CompilerParams(vmem_limit_bytes=26 * 1024 * 1024),
    )(returned, block_rows, gate_rows, up_rows, selection)
    return (token_grad, gate_wgrad, up_wgrad)


def solution(mesh):
    placed = (
        P(("expert", "shard"), None),
        P(("expert", "shard"), None),
        P("expert", None, "shard"),
        P("expert", None, "shard"),
        P("expert", None, "shard"),
        P("expert", None, "shard"),
        P("expert", None, "shard"),
    )
    small = mesh.shape["shard"] == 8 and mesh.shape["expert"] == 4
    return jax.shard_map(
        on_device if small else on_device_general,
        mesh=mesh,
        in_specs=placed,
        out_specs=(
            P(("expert", "shard"), None),
            P("expert", None, "shard"),
            P("expert", None, "shard"),
        ),
        check_vma=False,
    )
```

```python
import functools
import jax
import jax.numpy as jnp
from jax import lax
from jax.experimental import pallas as pl
from jax.experimental.pallas import tpu as pltpu
from jax.sharding import PartitionSpec as P

MESH = pl.DeviceIdType.MESH
UNITS = 4
GATHERS = 3
SUMS = 8
AHEAD = 2
STEPS = 19
ORDER = (
    ("multiply", 0, 1),
    ("token_forward", 2, 1),
    ("pair_sum", 1, 1),
    ("near_sum", 3, 1),
    ("token_spread", 4, 1),
    ("own_sum", 5, 1),
    ("spread", 9, 1),
    ("forward", 11, 1),
    ("token_pair", 14, 1),
    ("far", 14, 1),
    ("gathered", 16, 1),
    ("token_end", 16, 1),
)


def tiles_of(quarter):
    return (quarter // 2, quarter, quarter, quarter, quarter // 2)


def swiglu_grads(gate_values, up_values, hidden_cotangent):
    gate_float = gate_values.astype(jnp.float32)
    up_float = up_values.astype(jnp.float32)
    cotangent = hidden_cotangent.astype(jnp.float32)
    sigmoid_gate = jax.nn.sigmoid(gate_float)
    gate_grad = (
        cotangent * up_float * sigmoid_gate * (1.0 + gate_float * (1.0 - sigmoid_gate))
    ).astype(jnp.bfloat16)
    up_grad = (cotangent * gate_float * sigmoid_gate).astype(jnp.bfloat16)
    return (gate_grad, up_grad)


def slot_table(expert_ids, groups, capacity):
    token_count = expert_ids.shape[0]
    choices_per = expert_ids.shape[1]
    labels = lax.broadcasted_iota(jnp.int32, (1, 1, groups), 2)
    one_hot = (expert_ids[:, :, None] == labels).astype(jnp.int32)
    flat_hits = one_hot.reshape(token_count * choices_per, groups)
    earlier = jnp.cumsum(flat_hits, axis=0) - flat_hits
    slot_index = jnp.sum(flat_hits * earlier, axis=1).reshape(token_count, choices_per)
    slot_labels = lax.broadcasted_iota(jnp.int32, (1, 1, 1, capacity), 3)
    slot_hits = one_hot[:, :, :, None] * (slot_index[:, :, None, None] == slot_labels).astype(
        jnp.int32
    )
    selection = jnp.sum(slot_hits, axis=1).reshape(token_count, groups * capacity)
    return selection.astype(jnp.bfloat16)


def rows_inner(left_rows, right_rows):
    return lax.dot_general(
        left_rows, right_rows, (((0,), (0,)), ((), ())), preferred_element_type=jnp.float32
    )


def times_transposed(left_rows, weights):
    return lax.dot_general(
        left_rows, weights, (((1,), (1,)), ((), ())), preferred_element_type=jnp.float32
    )


def on_device_general(tokens, expert_ids, weight_gate, weight_up, gate_pre, up_pre, hidden_grad):
    groups = lax.axis_size("expert")
    shards = lax.axis_size("shard")
    model_width = tokens.shape[1]
    capacity = gate_pre.shape[1] // (groups * shards)
    selection = slot_table(expert_ids, groups, capacity)
    outgoing = rows_inner(selection, tokens).astype(jnp.bfloat16)
    gate_grad, up_grad = swiglu_grads(gate_pre[0], up_pre[0], hidden_grad[0])
    gate_matrix = weight_gate[0]
    up_matrix = weight_up[0]
    arrived = lax.all_to_all(
        outgoing.reshape(groups, capacity, model_width),
        "expert",
        split_axis=0,
        concat_axis=0,
        tiled=True,
    )
    block_rows = lax.all_gather(
        arrived.reshape(groups * capacity, model_width), "shard", axis=0, tiled=True
    )
    gate_rows = gate_grad
    up_rows = up_grad
    gate_wgrad = rows_inner(block_rows, gate_rows)
    up_wgrad = rows_inner(block_rows, up_rows)
    gate_rows = gate_grad
    up_rows = up_grad
    summed = lax.psum_scatter(
        (times_transposed(gate_rows, gate_matrix) + times_transposed(up_rows, up_matrix)).astype(
            jnp.bfloat16
        ),
        "shard",
        scatter_dimension=0,
        tiled=True,
    )
    outbound = summed.reshape(groups, capacity, model_width)
    returned = lax.all_to_all(outbound, "expert", split_axis=0, concat_axis=0, tiled=True)
    returned = returned.reshape(groups * capacity, model_width)
    token_grad = times_transposed(selection, returned.T).astype(jnp.bfloat16)
    return (token_grad, gate_wgrad[None], up_wgrad[None])


def slot_choice(expert_ids, groups, capacity):
    token_count = expert_ids.shape[1]
    lines = lax.broadcasted_iota(jnp.int32, (groups * capacity, token_count), 0)
    expert, slot = lines // capacity, lines % capacity
    named = jnp.logical_or(expert_ids[0:1, :] == expert, expert_ids[1:2, :] == expert)
    hits = jnp.where(named, 1.0, 0.0)
    above = lax.broadcasted_iota(jnp.int32, (token_count, token_count), 0)
    below = lax.broadcasted_iota(jnp.int32, (token_count, token_count), 1)
    before = jnp.where(above < below, 1.0, 0.0)
    earlier = jnp.dot(hits, before, preferred_element_type=jnp.float32)
    chosen = jnp.logical_and(named, earlier == slot.astype(jnp.float32))
    return jnp.where(chosen, 1.0, 0.0).astype(jnp.bfloat16)


def exchange_kernel(
    groups, capacity, expert_ids, tokens, weight_gate, weight_up, gate_pre, up_pre, hidden_grad,
    returned, block, gate_rows, up_rows, selection,
    choices, token_buf, outgoing, near_choices, near_tokens, near_outgoing, weights, pre, partial, from_core, total, from_diag,
    from_near, leaving, load_sem, send_sem, gather_sem, token_sem, sum_sem, return_sem,
):
    e = lax.axis_index("expert")
    q = lax.axis_index("shard")
    core, x, y = q % 2, (q // 2) % 2, q // 4
    sib = q + 1 - 2 * core
    xn = q + 2 - 4 * x
    yn = q + 4 - 8 * y
    dg = xn + 4 - 8 * y
    rows = groups * capacity
    half = rows // 2
    slots = gate_rows.shape[0]
    wide = block.shape[1] // UNITS
    slim = total.shape[2]
    tail = near_tokens.shape[2]
    late = slice(GATHERS * wide, GATHERS * wide + tail)
    peers = (q, xn, yn, dg)

    def columns(c, width):
        return pl.ds(pl.multiple_of(c * width, width), width)

    def span(start, size):
        return pl.ds(pl.multiple_of(start, size), size)

    def held(c, start, size):
        return block.at[span(start, size), columns(c, wide)]

    def chip_rows(c, device, low, size):
        return total.at[c, span(device // 2 * rows + low, size), :]

    def other(k):
        return (e + k) % groups

    def wait(place, sem):
        pltpu.make_async_copy(place, place, sem).wait()

    def target(k):
        if k < 3:
            return (other(k + 1), q)
        if k >= 18:
            return (other(k - 17), q)
        if k in (3, 7, 12, 14, 16):
            return (e, xn)
        if k in (4, 6, 13, 15, 17):
            return (e, yn)
        return (e, sib)

    def copy(k, c, piece=None):
        if k < 3:
            source = outgoing.at[other(k + 1), :, columns(c, wide)]
            to = held(c, q * rows + e * capacity, capacity)
        elif k < 6:
            source = to = held(c, q * rows, rows)
            if piece is not None:
                source = to = held(c, q * rows + other(piece) * capacity, capacity)
        elif k == 6:
            source = to = held(c, xn * rows, half)
        elif k == 7:
            source = to = held(c, yn * rows + half, half)
        elif k < 11:
            source = to = held(c, (xn, yn, dg)[k - 8] * rows, rows)
        elif k == 11:
            source, to = partial.at[c, 1 - core], from_core.at[c]
        elif k == 12:
            source, to = chip_rows(c, dg, 0, half), from_diag.at[c, 0]
        elif k == 13:
            source, to = chip_rows(c, dg, half, half), from_diag.at[c, 1]
        elif k == 14:
            source, to = chip_rows(c, xn, 0, half), from_near.at[c, 0, 0]
        elif k == 15:
            source, to = chip_rows(c, yn, half, half), from_near.at[c, 1, 1]
        elif k == 16:
            source, to = chip_rows(c, xn, half, half), from_near.at[c, 0, 1]
        elif k == 17:
            source, to = chip_rows(c, yn, 0, half), from_near.at[c, 1, 0]
        else:
            source = leaving.at[c, span(other(k - 17) * capacity, capacity), :]
            to = returned.at[span(e * capacity, capacity), columns(c, slim)]
        if k < 11:
            recv = gather_sem.at[c, (0, 0, 0, 1, 2, 4, 3, 3, 4, 4, 4)[k]]
        elif k < 18:
            recv = sum_sem.at[c, (0, 1, 1, 2, 2, 2, 2)[k - 11]]
        else:
            recv = return_sem.at[0]
        return pltpu.make_async_remote_copy(
            src_ref=source, dst_ref=to, send_sem=send_sem.at[0], recv_sem=recv,
            device_id=target(k), device_id_type=MESH,
        )

    def remote(source, to, recv, device, sent):
        return pltpu.make_async_remote_copy(
            src_ref=source, dst_ref=to, send_sem=send_sem.at[sent], recv_sem=token_sem.at[recv],
            device_id=device, device_id_type=MESH,
        )

    def announce():
        for i, peer in enumerate(peers[1:]):
            remote(choices, near_choices.at[i], 0, (e, peer), 1).start()
        for i, peer in enumerate((xn, yn)):
            remote(token_buf.at[:, late], near_tokens.at[i], 4 + i, (e, peer), 2).start()

    def token_forward(c):
        for i, peer in enumerate((yn, xn)):
            wait(near_tokens.at[i], token_sem.at[4 + i])
            here = slice(i * tail // 2, (i + 1) * tail // 2)
            remote(
                near_tokens.at[i, :, here], near_tokens.at[2, :, here], 1, (e, peer), 2
            ).start()

    def late_rows(peer, start, size):
        return block.at[span(peer * rows + start, size), late]

    def token_spread(c):
        wait(near_choices, token_sem.at[0])
        wait(near_tokens.at[2], token_sem.at[1])
        for i in range(3):
            picked = jnp.dot(
                slot_choice(near_choices[i], groups, capacity), near_tokens[i],
                preferred_element_type=jnp.float32,
            ).astype(jnp.bfloat16)
            for group in range(groups):
                near_outgoing[i, group] = picked[group * capacity : (group + 1) * capacity]
        for k in (1, 0, 2):
            for i, peer in enumerate(peers):
                if i == 0:
                    source = outgoing.at[other(k + 1), :, late]
                else:
                    source = near_outgoing.at[i - 1, other(k + 1)]
                to = late_rows(peer, e * capacity, capacity)
                remote(source, to, 2, (other(k + 1), q), 3).start()
        for i, peer in enumerate(peers[1:]):
            block[span(peer * rows + e * capacity, capacity), late] = near_outgoing[i, e]

    def token_pair(c):
        wait(block.at[pl.ds(0, 12 * capacity), late], token_sem.at[2])
        for peer in peers:
            place = late_rows(peer, 0, rows)
            remote(place, place, 3, (e, sib), 3).start()

    def token_end(c):
        wait(block.at[pl.ds(0, 4 * rows), late], token_sem.at[3])

    def weight_loads(c):
        for i, source in enumerate((weight_gate, weight_up)):
            pltpu.make_async_copy(
                source.at[0, columns(c, slim), :], weights.at[c, i], load_sem.at[c]
            ).start()

    token_load = pltpu.make_async_copy(tokens, token_buf, load_sem.at[SUMS])
    token_load.start()
    choice_load = pltpu.make_async_copy(expert_ids, choices, load_sem.at[SUMS + 2])
    choice_load.start()
    for i, source in enumerate((gate_pre, up_pre, hidden_grad)):
        pltpu.make_async_copy(source.at[0], pre.at[i], load_sem.at[SUMS + 1]).start()
    for c in range(AHEAD):
        weight_loads(c)

    barrier = pltpu.get_barrier_semaphore()
    for device in [(other(k), q) for k in (1, 2, 3)] + [(e, peer) for peer in (sib, xn, yn, dg)]:
        pl.semaphore_signal(barrier, inc=1, device_id=device, device_id_type=MESH)
    choice_load.wait()
    selection[...] = slot_choice(choices[...], groups, capacity)
    token_load.wait()
    for c in range(UNITS):
        here = slice(c * wide, (c + 1) * wide)
        picked = jnp.dot(
            selection[...], token_buf[:, here], preferred_element_type=jnp.float32
        ).astype(jnp.bfloat16)
        for group in range(groups):
            outgoing[group, :, here] = picked[group * capacity : (group + 1) * capacity]

    @pl.loop(0, UNITS)
    def _(c):
        here = columns(c, wide)
        block[span(q * rows + e * capacity, capacity), here] = outgoing[e, :, here]

    wait(pre, load_sem.at[SUMS + 1])
    step_rows = 32

    @pl.loop(0, slots // step_rows)
    def _(i):
        here = span(i * step_rows, step_rows)
        gate_grad, up_grad = swiglu_grads(pre[0, here, :], pre[1, here, :], pre[2, here, :])
        gate_rows[here, :] = gate_grad
        up_rows[here, :] = up_grad

    def products(c, low, size):
        term = times_transposed(gate_rows[low : low + size, :], weights[c, 0])
        term = term + times_transposed(up_rows[low : low + size, :], weights[c, 1])
        term = term.astype(jnp.bfloat16)
        for piece in range(size // rows):
            chip, side = divmod(low // rows + piece, 2)
            partial[c, side, chip * rows : (chip + 1) * rows, :] = term[
                piece * rows : (piece + 1) * rows
            ]

    def multiply(c):
        @pl.when(c < SUMS - AHEAD)
        def _():
            weight_loads(c + AHEAD)

        wait(weights.at[c], load_sem.at[c])
        products(c, 0, slots)
        copy(11, c).start()

    def spread(c):
        wait(held(c, 0, 3 * capacity), gather_sem.at[c, 0])
        for k in (3, 4):
            for piece in (1, 2, 3):
                copy(k, c, piece).start()
        copy(5, c).start()

    def forward(c):
        wait(held(c, 0, rows), gather_sem.at[c, 1])
        copy(6, c).start()
        copy(8, c).start()
        wait(held(c, 0, rows), gather_sem.at[c, 2])
        copy(7, c).start()
        copy(9, c).start()

    def far(c):
        wait(held(c, 0, rows), gather_sem.at[c, 3])
        copy(10, c).start()

    def gathered(c):
        wait(held(c, 0, 4 * rows), gather_sem.at[c, 4])

    def pair_sum(c):
        wait(from_core.at[c], sum_sem.at[c, 0])
        both = partial[c, core].astype(jnp.float32) + from_core[c].astype(jnp.float32)
        total[c] = both.astype(jnp.bfloat16)
        for k in (12, 13, 14, 15):
            copy(k, c).start()

    def near_sum(c):
        wait(from_diag.at[c], sum_sem.at[c, 1])
        for side, device, low in ((0, yn, 0), (1, xn, half)):
            place = span(device // 2 * rows + low, half)
            added = total[c, place, :].astype(jnp.float32) + from_diag[c, side].astype(jnp.float32)
            total[c, place, :] = added.astype(jnp.bfloat16)
            copy(17 if side == 0 else 16, c).start()

    def own_sum(c):
        wait(from_near.at[c], sum_sem.at[c, 2])
        for low in range(2):
            place = span(q // 2 * rows + low * half, half)
            added = total[c, place, :].astype(jnp.float32)
            added = added + from_near[c, 0, low].astype(jnp.float32)
            added = added + from_near[c, 1, low].astype(jnp.float32)
            leaving[c, low * half : (low + 1) * half, :] = added.astype(jnp.bfloat16)
        mine = span(e * capacity, capacity)
        returned[mine, columns(c, slim)] = leaving[c, mine, :]
        for k in (19, 18, 20):
            copy(k, c).start()

    weight_loads(AHEAD)
    wait(weights.at[0], load_sem.at[0])
    products(0, 0, slots // 2)
    pl.semaphore_wait(barrier, 7)
    announce()

    @pl.loop(0, GATHERS)
    def _(c):
        for k in (1, 0, 2):
            copy(k, c).start()
        for k in (3, 4):
            copy(k, c, 0).start()

    products(0, slots // 2, slots // 2)
    copy(11, 0).start()
    stages = dict(
        multiply=(multiply, SUMS), pair_sum=(pair_sum, SUMS), near_sum=(near_sum, SUMS),
        own_sum=(own_sum, SUMS), spread=(spread, GATHERS), forward=(forward, GATHERS),
        far=(far, GATHERS), gathered=(gathered, GATHERS), token_spread=(token_spread, 1),
        token_forward=(token_forward, 1), token_pair=(token_pair, 1), token_end=(token_end, 1),
    )

    @pl.loop(1, STEPS)
    def _(step):
        for name, first, every in ORDER:
            stage, count = stages[name]
            c = (step - first) // every
            ready = jnp.logical_and(step >= first, step < first + every * count)
            if every > 1:
                ready = jnp.logical_and(ready, (step - first) % every == 0)

            @pl.when(ready)
            def _():
                stage(c)

    wait(returned.at[pl.ds(0, 3 * capacity), :], return_sem.at[0])
    sent = (3 * capacity + 6 * rows + 2 * half) * GATHERS * wide
    sent = sent + (3 * capacity + 6 * half + slots // 2) * SUMS * slim
    wait(weight_gate.at[0, pl.ds(0, sent // weight_gate.shape[2]), :], send_sem.at[0])
    wait(near_choices, send_sem.at[1])
    wait(near_tokens, send_sem.at[2])
    wait(block.at[pl.ds(0, 12 * capacity + 4 * rows), late], send_sem.at[3])


def weight_grad_kernel(
    returned, block_rows, gate_rows, up_rows, selection, token_grad, gate_wgrad, up_wgrad,
    staged, token_staged, store_sem, token_sem,
):
    quarter = block_rows.shape[1] // 4
    tiles = tiles_of(quarter)
    stores = []
    low = 0
    for i, tile in enumerate(tiles):
        here = slice(low, low + tile)
        for j, (grads, wgrad) in enumerate(((gate_rows, gate_wgrad), (up_rows, up_wgrad))):
            if i >= 2:
                stores[2 * i + j - 4].wait()
            place = staged.at[i % 2, j, pl.ds(0, tile), :]
            place[...] = rows_inner(block_rows[:, here], grads[...])
            stores.append(
                pltpu.make_async_copy(place, wgrad.at[0, pl.ds(low, tile), :], store_sem.at[i % 2, j])
            )
            stores[-1].start()
        if i == 1:
            token_staged[...] = rows_inner(selection[...], returned[...]).astype(jnp.bfloat16)
            token_store = pltpu.make_async_copy(token_staged, token_grad, token_sem.at[0])
            token_store.start()
        low += tile
    for store in stores[-4:]:
        store.wait()
    token_store.wait()


def on_device(tokens, expert_ids, weight_gate, weight_up, gate_pre, up_pre, hidden_grad):
    groups = lax.axis_size("expert")
    shards = lax.axis_size("shard")
    token_count, model_width = tokens.shape
    slots, hidden = gate_pre.shape[1:]
    capacity = slots // (groups * shards)
    rows = groups * capacity
    slim = model_width // SUMS
    tail = model_width // UNITS * (UNITS - GATHERS)
    bf16 = jnp.bfloat16
    kept = [
        pltpu.with_memory_space_constraint(array, pltpu.HBM)
        for array in (expert_ids.T, tokens, weight_gate, weight_up, gate_pre, up_pre, hidden_grad)
    ]
    in_vmem = pl.BlockSpec(memory_space=pltpu.VMEM)
    in_hbm = pl.BlockSpec(memory_space=pltpu.HBM)
    returned, block_rows, gate_rows, up_rows, selection = pl.pallas_call(
        functools.partial(exchange_kernel, groups, capacity),
        out_shape=(
            jax.ShapeDtypeStruct((rows, model_width), bf16),
            jax.ShapeDtypeStruct((slots, model_width), bf16),
            jax.ShapeDtypeStruct((slots, hidden), bf16),
            jax.ShapeDtypeStruct((slots, hidden), bf16),
            jax.ShapeDtypeStruct((rows, token_count), bf16),
        ),
        in_specs=[in_hbm] * 7,
        out_specs=(in_vmem,) * 5,
        scratch_shapes=[
            pltpu.VMEM(expert_ids.shape[::-1], expert_ids.dtype),
            pltpu.VMEM((token_count, model_width), bf16),
            pltpu.VMEM((groups, capacity, model_width), bf16),
            pltpu.VMEM((3, *expert_ids.shape[::-1]), expert_ids.dtype),
            pltpu.VMEM((3, token_count, tail), bf16),
            pltpu.VMEM((3, groups, capacity, tail), bf16),
            pltpu.VMEM((SUMS, 2, slim, hidden), bf16),
            pltpu.VMEM((3, slots, hidden), bf16),
            pltpu.VMEM((SUMS, 2, slots // 2, slim), bf16),
            pltpu.VMEM((SUMS, slots // 2, slim), bf16),
            pltpu.VMEM((SUMS, slots // 2, slim), bf16),
            pltpu.VMEM((SUMS, 2, rows // 2, slim), bf16),
            pltpu.VMEM((SUMS, 2, 2, rows // 2, slim), bf16),
            pltpu.VMEM((SUMS, rows, slim), bf16),
            pltpu.SemaphoreType.DMA((SUMS + 3,)),
            pltpu.SemaphoreType.DMA((4,)),
            pltpu.SemaphoreType.DMA((GATHERS, 5)),
            pltpu.SemaphoreType.DMA((6,)),
            pltpu.SemaphoreType.DMA((SUMS, 3)),
            pltpu.SemaphoreType.DMA((1,)),
        ],
        compiler_params=pltpu.CompilerParams(
            collective_id=0, has_side_effects=True, vmem_limit_bytes=40 * 1024 * 1024
        ),
    )(*kept)
    wgrad_shape = jax.ShapeDtypeStruct((1, model_width, hidden), jnp.float32)
    token_grad, gate_wgrad, up_wgrad = pl.pallas_call(
        weight_grad_kernel,
        out_shape=(jax.ShapeDtypeStruct((token_count, model_width), bf16), wgrad_shape, wgrad_shape),
        in_specs=[in_vmem] * 5,
        out_specs=(in_hbm,) * 3,
        scratch_shapes=[
            pltpu.VMEM((2, 2, model_width // 4, hidden), jnp.float32),
            pltpu.VMEM((token_count, model_width), bf16),
            pltpu.SemaphoreType.DMA((2, 2)),
            pltpu.SemaphoreType.DMA((1,)),
        ],
        compiler_params=pltpu.CompilerParams(vmem_limit_bytes=26 * 1024 * 1024),
    )(returned, block_rows, gate_rows, up_rows, selection)
    return (token_grad, gate_wgrad, up_wgrad)


def solution(mesh):
    placed = (
        P(("expert", "shard"), None),
        P(("expert", "shard"), None),
        P("expert", None, "shard"),
        P("expert", None, "shard"),
        P("expert", None, "shard"),
        P("expert", None, "shard"),
        P("expert", None, "shard"),
    )
    small = mesh.shape["shard"] == 8 and mesh.shape["expert"] == 4
    return jax.shard_map(
        on_device if small else on_device_general,
        mesh=mesh,
        in_specs=placed,
        out_specs=(
            P(("expert", "shard"), None),
            P("expert", None, "shard"),
            P("expert", None, "shard"),
        ),
        check_vma=False,
    )
```
